256 devices in a mesh: gx: 8 (over x_lo, y), gy: 32 (over x_hi, z, core).
Axes of the slice: x: 4 (x_hi: 2, x_lo: 2; x = x_hi * 2 + x_lo), y: 4, z: 8, core: 2. Of those that a mesh axis runs over, the one named last changes fastest.
Arguments:
- positions: float32 [3, 524288], P(None, ('gx', 'gy')), may hold values from 0 to 4
- node_moments: float32 [10, 131072], P(None, ('gx', 'gy')), as said below
- slot_of: int32 [256, 2048], P(('gx', 'gy')), may hold values from 0 to 2047, each once within a row
- block_list: int32 [4096, 16], P(('gx', 'gy')), may hold values from 0 to 1023, as said below
- tile_counts: int32 [4096], P(('gx', 'gy')), may hold values from 1 to 16, as said below
Outputs:
- accel: float32 [3, 524288], P(None, ('gx', 'gy'))
The draws below stay inside these ranges and needn't reach their ends.
Inputs may be any that keep to these rules, and one draw needn't show every extreme that they name: `block_list`: each row names 16 different node blocks; only a tile's first tile_counts entries are used. `tile_counts`: some tile of every draw uses all 16 slots. `node_moments`: masses lie in 0.02 to 0.2 and centres in 0 to 4.
All inputs are finite; a program needn't handle non-finite values.
Results may differ from the reference program's by a relative error of at most 0.0003.
Values sent between devices are 32-bit elements; how exact they have to be, the bound alone decides.
A program may use at most 64 MiB of HBM per device.

```python
import math
import jax
import jax.numpy as jnp
from jax import lax

PART_DEV = 2048
TILE = 128
BLOCK = 128
LIST = 16
TILES_DEV = 16
TILES = 4096
PARTS_SIZE = 524288
NODES = 131072
DEVICES = 256


def draw_node_moments(key, part):
    mass_key = jax.random.fold_in(key, 11)
    centre_key = jax.random.fold_in(key, 12)
    quad_key = jax.random.fold_in(key, 13)
    mass = jnp.exp(jax.random.uniform(mass_key, (1, NODES), jnp.float32, math.log(0.02), math.log(0.2)))
    centre = jax.random.uniform(centre_key, (3, NODES), jnp.float32, 0.0, 4.0)
    quad = 0.05 * jax.random.normal(quad_key, (6, NODES), jnp.float32)
    return jnp.concatenate([mass, centre, quad], axis=0).astype(jnp.float32)


def draw_block_list(key, part):
    score_key = jax.random.fold_in(key, 21)
    total_blocks = NODES // BLOCK
    scores = jax.random.randint(score_key, (TILES, total_blocks), 0, 2 ** 18, jnp.int32)
    scores = scores * total_blocks + jnp.arange(total_blocks, dtype=jnp.int32)[None, :]
    chosen = jax.lax.top_k(scores, LIST)[1]
    return chosen.astype(jnp.int32)


def draw_tile_counts(key, part):
    level_key = jax.random.fold_in(key, 31)
    count_key = jax.random.fold_in(key, 32)
    level = jax.random.randint(level_key, (DEVICES, 1), max(LIST // 4, 1), LIST + 1, jnp.int32)
    counts = jax.random.randint(count_key, (DEVICES, TILES_DEV), 1, level + 1, jnp.int32)
    counts = counts.at[0, 0].set(LIST)
    return counts.reshape(TILES).astype(jnp.int32)


def steps_of(rng, extent, cuts, low, largest):
    factor_of = 1.0
    for position, shards_of in cuts:
        steps = jax.random.uniform(jax.random.fold_in(jax.random.fold_in(rng, 6), position), (shards_of,), jnp.float32, low / len(cuts), largest / len(cuts))
        factor_of = factor_of * jnp.repeat(jnp.exp(steps), extent[position] // shards_of).reshape((-1,) + (1,) * (len(extent) - 1 - position))
    return factor_of


def setup_inputs(seed: int = 0) -> dict:
    streams_of = jax.random.split(jax.random.key(seed), 6)
    positions = jnp.clip(4.0 * jax.random.uniform(streams_of[0], (3, PARTS_SIZE), jnp.float32) ** steps_of(streams_of[0], (3, PARTS_SIZE), ((1, 256),), -0.2, 0.2), 0.0, 4.0)
    node_moments = draw_node_moments(jax.random.fold_in(streams_of[5], 71), 0)
    slot_of = jax.vmap(lambda own: jax.random.permutation(own, PART_DEV))(jax.random.split(streams_of[2], DEVICES)).reshape((DEVICES, PART_DEV)).astype(jnp.int32)
    block_list = draw_block_list(jax.random.fold_in(streams_of[5], 71), 0)
    tile_counts = draw_tile_counts(jax.random.fold_in(streams_of[5], 71), 0)
    return {"positions": positions, "node_moments": node_moments, "slot_of": slot_of, "block_list": block_list, "tile_counts": tile_counts}


split_a = 0.5
soft_sq = 0.25

def pair_sum(tiled, near):
    delta = tiled[:, :, :, None] - near[1:4, :, None, :]
    mass = near[0][:, None, :]
    qxx = near[4][:, None, :]
    qyy = near[5][:, None, :]
    qzz = near[6][:, None, :]
    qxy = near[7][:, None, :]
    qxz = near[8][:, None, :]
    qyz = near[9][:, None, :]
    dxv = delta[0]
    dyv = delta[1]
    dzv = delta[2]
    dist_sq = dxv * dxv + dyv * dyv + dzv * dzv + soft_sq
    dist = jnp.sqrt(dist_sq)
    expo = jnp.exp(-split_a * split_a * dist_sq)
    root_pi = math.sqrt(math.pi)
    zeroth = jax.scipy.special.erfc(split_a * dist) / dist
    first = (zeroth + 2.0 * split_a / root_pi * expo) / dist_sq
    second = (3.0 * first + 4.0 * split_a ** 3 / root_pi * expo) / dist_sq
    third = (5.0 * second + 8.0 * split_a ** 5 / root_pi * expo) / dist_sq
    quad_x = qxx * dxv + qxy * dyv + qxz * dzv
    quad_y = qxy * dxv + qyy * dyv + qyz * dzv
    quad_z = qxz * dxv + qyz * dyv + qzz * dzv
    inner = dxv * quad_x + dyv * quad_y + dzv * quad_z
    radial = -mass * first - 0.5 * third * inner + 0.5 * second * (qxx + qyy + qzz)
    force_x = lax.optimization_barrier(jnp.sum(radial * dxv + second * quad_x, axis=-1))
    force_y = lax.optimization_barrier(jnp.sum(radial * dyv + second * quad_y, axis=-1))
    force_z = lax.optimization_barrier(jnp.sum(radial * dzv + second * quad_z, axis=-1))
    return jnp.stack([force_x, force_y, force_z])

def tile_forces(tiled, blocks, lists, counts, trips):

    def slot_term(step, total):
        ids = lax.dynamic_index_in_dim(lists, step, 1, keepdims=False)
        near = jnp.take(blocks, ids, axis=1)
        live = (step < counts).astype(jnp.float32)
        return total + pair_sum(tiled, near) * live[None, :, None]
    start = jnp.zeros(tiled.shape, jnp.float32)
    return lax.fori_loop(0, trips, slot_term, start)

def reference(positions, node_moments, slot_of, block_list, tile_counts):
    blocks = node_moments.reshape(10, -1, BLOCK)
    own_pos = jnp.transpose(positions.reshape(3, DEVICES, PART_DEV), (1, 0, 2))
    own_lists = block_list.reshape(DEVICES, TILES_DEV, LIST)
    own_counts = tile_counts.reshape(DEVICES, TILES_DEV)

    def one_device(items):
        pos, slots, lists, counts = items
        tiled = jnp.zeros(pos.shape, jnp.float32).at[:, slots].set(pos).reshape(3, TILES_DEV, TILE)
        forces = tile_forces(tiled, blocks, lists, counts, LIST).reshape(3, PART_DEV)
        return forces[:, slots]
    result = lax.map(one_device, (own_pos, slot_of, own_lists, own_counts))
    return jnp.transpose(result, (1, 0, 2)).reshape(3, DEVICES * PART_DEV)
```

```python
import functools
import math

import jax
import jax.numpy as jnp
from jax import lax
from jax.experimental import pallas as pl
from jax.experimental.pallas import tpu as pltpu
from jax.sharding import PartitionSpec as P

MESH = pl.DeviceIdType.MESH
NZ = 8
NR = 4

def device_of(first, p, q, z, c):
    x = first * p + (1 - first) * q
    y = first * q + (1 - first) * p
    return (lax.rem(x, 2) * 4 + y, (x // 2) * 16 + z * 2 + c)

def gather_kernel(own_ref, v3, v2, pin_sem, zin_sem, qin_sem, cin_sem, psend, zsend, qsend, csend, own_sem):
    gx = lax.axis_index("gx")
    gy = lax.axis_index("gy")
    c = lax.rem(gy, 2)
    z = lax.rem(gy // 2, 8)
    x = (gy // 16) * 2 + gx // 4
    y = lax.rem(gx, 4)
    refs = (v3, v2)
    rows = ((0, 24), (24, 16))
    firsts = (1 - c, c)
    ps = tuple(f * x + (1 - f) * y for f in firsts)
    qs = tuple(f * y + (1 - f) * x for f in firsts)

    def dev(s, p, q, zz, cc):
        return device_of(firsts[s], lax.rem(p, 4), lax.rem(q, 4), lax.rem(zz, 8), cc)

    def zat(rel):
        return lax.rem(z + rel, 8)

    def qat(s, rel):
        return lax.rem(qs[s] + rel, 4)

    barrier = pltpu.get_barrier_semaphore()
    peers = []
    for dx in (1, 2, 3):
        peers.append(device_of(1, lax.rem(x + dx, 4), y, z, c))
        peers.append(device_of(1, x, lax.rem(y + dx, 4), z, c))
    for dz in range(1, 8):
        peers.append(device_of(1, x, y, lax.rem(z + dz, 8), c))
    peers.append(device_of(1, x, y, z, 1 - c))
    for peer in peers:
        pl.semaphore_signal(barrier, inc=1, device_id=peer, device_id_type=MESH)
    own = []
    for s in (0, 1):
        r0, rn = rows[s]
        cp = pltpu.make_async_copy(own_ref.at[pl.ds(r0, rn)], refs[s].at[c, qs[s], z, ps[s]], own_sem.at[s])
        cp.start()
        own.append(cp)
    pl.semaphore_wait(barrier, len(peers))

    sends = []

    def send(src, dst, ssem, rsem, to):
        cp = pltpu.make_async_remote_copy(src_ref=src, dst_ref=dst, send_sem=ssem, recv_sem=rsem, device_id=to, device_id_type=MESH)
        cp.start()
        sends.append(cp)

    def arrived(ref, sem):
        pltpu.make_async_remote_copy(src_ref=ref, dst_ref=ref, send_sem=sem, recv_sem=sem, device_id=(gx, gy), device_id_type=MESH).wait_recv()

    for s in (0, 1):
        r0, rn = rows[s]
        unit = refs[s].at[c, qs[s], z, ps[s]]
        src = own_ref.at[pl.ds(r0, rn)]
        for d in (1, 7, 2, 6, 3, 5, 4):
            send(src, unit, zsend.at[s, d], zin_sem.at[s, d], dev(s, ps[s], qs[s], z + d, c))
        for i, d in enumerate((1, 3, 2)):
            send(src, unit, psend.at[s, 0, i], pin_sem.at[s, 0, i], dev(s, ps[s] + d, qs[s], z, c))
    for cp in own:
        cp.wait()

    def bundle(s, qrel, zrel):
        return refs[s].at[c, qat(s, qrel), zat(zrel)]

    def column(zrel):
        for s in (0, 1):
            u = refs[s].at[c, qs[s], zat(zrel), ps[s]]
            arrived(u, zin_sem.at[s, 8 - zrel])
            for i, d in enumerate((1, 3, 2)):
                send(u, u, psend.at[s, zrel, i], pin_sem.at[s, zrel, i], dev(s, ps[s] + d, qs[s], z, c))

    def ready(zrel):
        for s in (0, 1):
            for i, d in enumerate((1, 3, 2)):
                arrived(refs[s].at[c, qs[s], zat(zrel), lax.rem(ps[s] + 4 - d, 4)], pin_sem.at[s, zrel, i])
            b = bundle(s, 0, zrel)
            send(b, b, qsend.at[s, zrel, 0], qin_sem.at[s, zrel, 0], dev(s, ps[s], qs[s] + 1, z, c))
            send(b, b, qsend.at[s, zrel, 1], qin_sem.at[s, zrel, 1], dev(s, ps[s], qs[s] + 3, z, c))
            send(b, b, csend.at[s, zrel, 0], cin_sem.at[s, zrel, 0], dev(s, ps[s], qs[s], z, 1 - c))

    def side(zrel):
        for s in (0, 1):
            for i, rel in ((0, 3), (1, 1)):
                b = bundle(s, rel, zrel)
                arrived(b, qin_sem.at[s, zrel, i])
                h = b.at[pl.ds(2 * i, 2)]
                send(h, h, qsend.at[s, zrel, 2 + i], qin_sem.at[s, zrel, 2 + i], dev(s, ps[s], qs[s] + (1 if i == 0 else 3), z, c))
                send(b, b, csend.at[s, zrel, 1 + i], cin_sem.at[s, zrel, 1 + i], dev(s, ps[s], qs[s], z, 1 - c))

    def far(zrel):
        for s in (0, 1):
            b = bundle(s, 2, zrel)
            for i in (0, 1):
                arrived(b.at[pl.ds(2 * i, 2)], qin_sem.at[s, zrel, 2 + i])
            send(b, b, csend.at[s, zrel, 3], cin_sem.at[s, zrel, 3], dev(s, ps[s], qs[s], z, 1 - c))

    column(1)
    column(7)
    ready(0)
    column(2)
    column(6)
    column(3)
    column(5)
    column(4)
    ready(1)
    ready(7)
    side(0)
    ready(2)
    ready(6)
    side(1)
    side(7)
    far(0)
    ready(3)
    ready(5)
    side(2)
    side(6)
    far(1)
    far(7)
    ready(4)
    side(3)
    side(5)
    far(2)
    far(6)
    side(4)
    far(3)
    far(5)
    far(4)
    for s in (0, 1):
        for zrel in (0, 1, 7, 2, 6, 3, 5, 4):
            for k, qrel in enumerate((0, 3, 1, 2)):
                qp = lax.rem(qs[1 - s] + qrel, 4)
                arrived(refs[s].at[1 - c, qp, zat(zrel)], cin_sem.at[s, zrel, k])
    for cp in sends:
        cp.wait_send()

def gather_nodes(own, out_space=pltpu.VMEM):
    dma = pltpu.SemaphoreType.DMA
    return pl.pallas_call(
        gather_kernel,
        out_shape=[jax.ShapeDtypeStruct((2, NR, NZ, NR, 24, 128), jnp.float32),
                   jax.ShapeDtypeStruct((2, NR, NZ, NR, 16, 128), jnp.float32)],
        in_specs=[pl.BlockSpec(memory_space=pltpu.VMEM)],
        out_specs=[pl.BlockSpec(memory_space=out_space)] * 2,
        scratch_shapes=[dma((2, 8, 3)), dma((2, 8)), dma((2, 8, 4)), dma((2, 8, 4)),
                        dma((2, 8, 3)), dma((2, 8)), dma((2, 8, 4)), dma((2, 8, 4)), dma((2,))],
        compiler_params=pltpu.CompilerParams(collective_id=0, has_side_effects=True, vmem_limit_bytes=40 << 20),
        name="gather_nodes",
    )(own)


F32 = jnp.float32
BF16 = jnp.bfloat16
TILE = 128
TILES = 16
LIST = 16
RADIAL = (4.85670015e-05, -0.00186169315, 1.72317441, -0.284668104, 5.03335967, -6.00634052, 5.41671318,
          -3.57716793, 1.66240908, -0.511649185, 0.0932067366, -0.00758405181)
ROOT_PI = math.sqrt(math.pi)
K1 = 0.5 / ROOT_PI
K2_FIFTH = 0.25 / ROOT_PI / 5.0
EXP_RATE = -0.25 * math.log2(math.e)

def thirds(v):
    a = v.astype(BF16)
    r = v - a.astype(F32)
    b = r.astype(BF16)
    return a, b, (r - b.astype(F32)).astype(BF16)

def halves(v):
    a = v.astype(BF16)
    return a, (v - a.astype(F32)).astype(BF16)

def particle_rows(pos):
    x = pos[0:1] - 2.0
    y = pos[1:2] - 2.0
    z = pos[2:3] - 2.0
    none = jnp.zeros_like(x)
    xx, yy, zz = x * x, y * y, z * z
    dist = [-2.0 * x, -2.0 * y, -2.0 * z, none + 1.0, xx + yy + zz] + [none] * 11
    quad = [none] * 5 + [5.0 * x, 5.0 * y, 5.0 * z, none - 2.5, -2.5 * (xx - zz), -2.5 * (yy - zz), -2.5 * zz,
            -5.0 * (x * y), -5.0 * (x * z), -5.0 * (y * z), none]
    return jnp.concatenate(dist + quad, axis=0)

def node_rows(v):
    mass = v[0]
    x, y, z = v[1] - 2.0, v[2] - 2.0, v[3] - 2.0
    qxx, qyy, qzz, qxy, qxz, qyz = v[4:]
    qcx = qxx * x + qxy * y + qxz * z
    qcy = qxy * x + qyy * y + qyz * z
    qcz = qxz * x + qyz * y + qzz * z
    return [x, y, z, x * x + y * y + z * z + 0.25, jnp.ones_like(x), qcx, qcy, qcz,
            x * qcx + y * qcy + z * qcz, qxx, qyy, qxx + qyy + qzz, qxy, qxz, qyz, mass]

def force_kernel(counts, lists, pos_ref, slot_ref, v3, v2, out_ref,
                 nodes, rows_p, slot16, slot_col, feats, where_p, sb, cols, rb, total, forces):
    lane = lax.broadcasted_iota(jnp.int32, (128, 128), 1)
    def node_step(i, _):
        c, q, z, p = i // 64, (i // 16) % 4, (i // 2) % 8, (i % 2) * 2
        vals = []
        for k in range(10):
            if k < 6:
                a, b = v3[c, q, z, p, 4 * k:4 * k + 4, :], v3[c, q, z, p + 1, 4 * k:4 * k + 4, :]
            else:
                a, b = v2[c, p, z, q, 4 * k - 24:4 * k - 20, :], v2[c, p + 1, z, q, 4 * k - 24:4 * k - 20, :]
            vals.append(jnp.concatenate([a, b], axis=0))
        for f, row in enumerate(node_rows(vals)):
            nodes[pl.ds(i * 128 + f, 8, stride=16), :] = row
        return 0
    lax.fori_loop(0, 128, node_step, 0)
    for r in range(16):
        slot16[r:r + 1, :] = slot_ref[0:1, r * 128:(r + 1) * 128]
    slot_t = slot16[...].T
    for r in range(16):
        slot_col[r] = jnp.broadcast_to(slot_t[:, r:r + 1], (128, 128))
    for i, piece in enumerate(thirds(particle_rows(pos_ref[...]))):
        rows_p[i * 32:(i + 1) * 32, :] = piece
    def tile_step(t, _):
        base = lane + t * 128
        acc = jnp.zeros((96, 128), F32)
        for r in range(0, 16, 2):
            hot = jnp.concatenate([(slot_col[r + h] == base).astype(F32).astype(BF16) for h in (0, 1)], axis=0)
            acc = acc + jnp.dot(rows_p[:, r * 128:(r + 2) * 128], hot, preferred_element_type=F32)
        got = acc.astype(BF16)
        for g, piece in enumerate((0, 0, 0, 1, 1, 2)):
            feats[t, g * 16:(g + 1) * 16, 0:128] = got[piece * 32:piece * 32 + 16]
            feats[t, g * 16:(g + 1) * 16, 128:256] = got[piece * 32 + 16:piece * 32 + 32]
        where_p[t] = -0.5 * (acc[0:8] + acc[32:40] + acc[64:72])
        return 0
    lax.fori_loop(0, TILES, tile_step, 0)
    total[...] = jnp.zeros_like(total)
    rb[...] = jnp.zeros_like(rb)
    sb[...] = jnp.ones_like(sb)
    cols[...] = jnp.zeros_like(cols)

    def block_row(b):
        d = b // 4
        gx, gy = d // 32, d % 32
        c, z = gy % 2, (gy // 2) % 8
        x, y = (gy // 16) * 2 + gx // 4, gx % 4
        p = jnp.where(c == 0, x, y)
        q = jnp.where(c == 0, y, x)
        return ((((c * 4 + q) * 8 + z) * 4 + p) * 4 + b % 4) * 16

    live = lax.fori_loop(0, TILES, lambda t, n: n + counts[t], 0)

    def pair_step(i, carry):
        t0, k0, row1, t1, row2, t2 = carry
        hi, lo = halves(nodes[pl.ds(pl.multiple_of(row2, 16), 16), :])
        left = jnp.concatenate([jnp.concatenate([hi, hi], axis=1), jnp.concatenate([lo, lo], axis=1)], axis=0)
        total[t2] += jnp.dot(left, rb[...], preferred_element_type=F32)
        for r in range(0, 128, 16):
            s2 = sb[r:r + 16, 0:128]
            inner = sb[r:r + 16, 128:256]
            mass = jnp.broadcast_to(cols[r:r + 16, 15:16], (16, 128)) * (-1.0 / 3.0)
            trace = jnp.broadcast_to(cols[r:r + 16, 11:12], (16, 128)) * 0.5
            w = lax.rsqrt(s2)
            e = jnp.exp2(s2 * EXP_RATE)
            a1 = jnp.full_like(w, RADIAL[-1])
            for coef in RADIAL[-2::-1]:
                a1 = a1 * w + coef
            u = w * w
            g2 = (a1 + K1) * u
            g3 = (g2 + K2_FIFTH) * u
            radial = e * (mass * a1 + trace * g2 + inner * g3)
            second = e * g2
            hi, lo = halves(radial)
            rb[r:r + 16, 0:128] = hi
            rb[128 + r:128 + r + 16, 0:128] = lo
            hi, lo = halves(second)
            rb[r:r + 16, 128:256] = hi
            rb[128 + r:128 + r + 16, 128:256] = lo
        ok = i < live
        t = jnp.minimum(t0, TILES - 1)
        row0 = block_row(jnp.where(ok, lists[t, k0], 0))
        node = nodes[pl.ds(pl.multiple_of(row0, 16), 16), :]
        p1, p2, p3 = thirds(node)
        stack = jnp.concatenate([p1, p2, p3, p1, p2, p1], axis=0)
        cols[:, 0:16] = node.T
        sb[...] = jnp.dot(stack.T, feats[t], preferred_element_type=F32)
        tt = jnp.where(ok, t, TILES)
        last = k0 + 1 >= counts[t]
        return (jnp.where(last, t0 + 1, t0), jnp.where(last, 0, k0 + 1), row0, tt, row1, t1)
    lax.fori_loop(0, live + 2, pair_step, (0, 0, 0, TILES, 0, TILES))

    for t in range(TILES):
        s = total[t, 0:16, :] + total[t, 16:32, :]
        x, y, z = where_p[t, 0:1, :], where_p[t, 1:2, :], where_p[t, 2:3, :]
        rad = lambda k: s[k:k + 1, 0:128]
        sec = lambda k: s[k:k + 1, 128:256]
        m = rad(4)
        xx, yy, xy, xz, yz = sec(9), sec(10), sec(12), sec(13), sec(14)
        zz = sec(11) - xx - yy
        forces[0, t:t + 1, :] = x * m - rad(0) + xx * x + xy * y + xz * z - sec(5)
        forces[1, t:t + 1, :] = y * m - rad(1) + xy * x + yy * y + yz * z - sec(6)
        forces[2, t:t + 1, :] = z * m - rad(2) + xz * x + yz * y + zz * z - sec(7)
    slot = slot16[...]
    at = slot % 128
    tile = slot // 128
    for k in range(3):
        got = jnp.zeros((16, 128), F32)
        for t in range(TILES):
            row = jnp.broadcast_to(forces[k, t:t + 1, :], (16, 128))
            got = jnp.where(tile == t, jnp.take_along_axis(row, at, axis=1), got)
        for r in range(16):
            out_ref[k:k + 1, r * 128:(r + 1) * 128] = got[r:r + 1, :]

def forces_of(counts, lists, pos, slots, v3, v2):
    vmem = pl.BlockSpec(memory_space=pltpu.VMEM)
    smem = pl.BlockSpec(memory_space=pltpu.SMEM)
    return pl.pallas_call(
        force_kernel,
        out_shape=jax.ShapeDtypeStruct(pos.shape, F32),
        in_specs=[smem, smem, vmem, vmem, vmem, vmem],
        out_specs=vmem,
        scratch_shapes=[pltpu.VMEM((1024 * 16, 128), F32), pltpu.VMEM((96, 2048), BF16), pltpu.VMEM((16, 128), jnp.int32),
                        pltpu.VMEM((16, 128, 128), jnp.int32), pltpu.VMEM((16, 96, 256), BF16), pltpu.VMEM((16, 8, 128), F32),
                        pltpu.VMEM((128, 256), F32), pltpu.VMEM((128, 128), F32), pltpu.VMEM((256, 256), BF16),
                        pltpu.VMEM((17, 32, 256), F32), pltpu.VMEM((3, 16, 128), F32)],
        compiler_params=pltpu.CompilerParams(vmem_limit_bytes=24 << 20),
        name="tile_forces",
    )(counts, lists, pos, slots, v3, v2)


def shards(positions, node_moments, slot_of, block_list, tile_counts):
    own = node_moments.reshape(40, 128)
    v3, v2 = gather_nodes(own)
    return forces_of(tile_counts, block_list, positions, slot_of, v3, v2)


def solution(mesh):
    placed = (
        P(None, ("gx", "gy")),
        P(None, ("gx", "gy")),
        P(("gx", "gy"), None),
        P(("gx", "gy"), None),
        P(("gx", "gy")),
    )
    return jax.shard_map(
        shards, mesh=mesh, in_specs=placed, out_specs=P(None, ("gx", "gy")), check_vma=False
    )
```

```python
import functools
import math

import jax
import jax.numpy as jnp
from jax import lax
from jax.experimental import pallas as pl
from jax.experimental.pallas import tpu as pltpu
from jax.sharding import PartitionSpec as P

MESH = pl.DeviceIdType.MESH
NZ = 8
NR = 4

def device_of(first, p, q, z, c):
    x = first * p + (1 - first) * q
    y = first * q + (1 - first) * p
    return (lax.rem(x, 2) * 4 + y, (x // 2) * 16 + z * 2 + c)

def gather_kernel(own_ref, v3, v2, pin_sem, zin_sem, qin_sem, cin_sem, psend, zsend, qsend, csend, own_sem):
    gx = lax.axis_index("gx")
    gy = lax.axis_index("gy")
    c = lax.rem(gy, 2)
    z = lax.rem(gy // 2, 8)
    x = (gy // 16) * 2 + gx // 4
    y = lax.rem(gx, 4)
    refs = (v3, v2)
    rows = ((0, 24), (24, 16))
    firsts = (1 - c, c)
    ps = tuple(f * x + (1 - f) * y for f in firsts)
    qs = tuple(f * y + (1 - f) * x for f in firsts)

    def dev(s, p, q, zz, cc):
        return device_of(firsts[s], lax.rem(p, 4), lax.rem(q, 4), lax.rem(zz, 8), cc)

    def zat(rel):
        return lax.rem(z + rel, 8)

    def qat(s, rel):
        return lax.rem(qs[s] + rel, 4)

    barrier = pltpu.get_barrier_semaphore()
    peers = []
    for dx in (1, 2, 3):
        peers.append(device_of(1, lax.rem(x + dx, 4), y, z, c))
        peers.append(device_of(1, x, lax.rem(y + dx, 4), z, c))
    for dz in range(1, 8):
        peers.append(device_of(1, x, y, lax.rem(z + dz, 8), c))
    peers.append(device_of(1, x, y, z, 1 - c))
    for peer in peers:
        pl.semaphore_signal(barrier, inc=1, device_id=peer, device_id_type=MESH)
    own = []
    for s in (0, 1):
        r0, rn = rows[s]
        cp = pltpu.make_async_copy(own_ref.at[pl.ds(r0, rn)], refs[s].at[c, qs[s], z, ps[s]], own_sem.at[s])
        cp.start()
        own.append(cp)
    pl.semaphore_wait(barrier, len(peers))

    sends = []

    def send(src, dst, ssem, rsem, to):
        cp = pltpu.make_async_remote_copy(src_ref=src, dst_ref=dst, send_sem=ssem, recv_sem=rsem, device_id=to, device_id_type=MESH)
        cp.start()
        sends.append(cp)

    def arrived(ref, sem):
        pltpu.make_async_remote_copy(src_ref=ref, dst_ref=ref, send_sem=sem, recv_sem=sem, device_id=(gx, gy), device_id_type=MESH).wait_recv()

    for s in (0, 1):
        r0, rn = rows[s]
        unit = refs[s].at[c, qs[s], z, ps[s]]
        src = own_ref.at[pl.ds(r0, rn)]
        for d in (1, 7, 2, 6, 3, 5, 4):
            send(src, unit, zsend.at[s, d], zin_sem.at[s, d], dev(s, ps[s], qs[s], z + d, c))
        for i, d in enumerate((1, 3, 2)):
            send(src, unit, psend.at[s, 0, i], pin_sem.at[s, 0, i], dev(s, ps[s] + d, qs[s], z, c))
    for cp in own:
        cp.wait()

    def bundle(s, qrel, zrel):
        return refs[s].at[c, qat(s, qrel), zat(zrel)]

    def column(zrel):
        for s in (0, 1):
            u = refs[s].at[c, qs[s], zat(zrel), ps[s]]
            arrived(u, zin_sem.at[s, 8 - zrel])
            for i, d in enumerate((1, 3, 2)):
                send(u, u, psend.at[s, zrel, i], pin_sem.at[s, zrel, i], dev(s, ps[s] + d, qs[s], z, c))

    def ready(zrel):
        for s in (0, 1):
            for i, d in enumerate((1, 3, 2)):
                arrived(refs[s].at[c, qs[s], zat(zrel), lax.rem(ps[s] + 4 - d, 4)], pin_sem.at[s, zrel, i])
            b = bundle(s, 0, zrel)
            send(b, b, qsend.at[s, zrel, 0], qin_sem.at[s, zrel, 0], dev(s, ps[s], qs[s] + 1, z, c))
            send(b, b, qsend.at[s, zrel, 1], qin_sem.at[s, zrel, 1], dev(s, ps[s], qs[s] + 3, z, c))
            send(b, b, csend.at[s, zrel, 0], cin_sem.at[s, zrel, 0], dev(s, ps[s], qs[s], z, 1 - c))

    def side(zrel):
        for s in (0, 1):
            for i, rel in ((0, 3), (1, 1)):
                b = bundle(s, rel, zrel)
                arrived(b, qin_sem.at[s, zrel, i])
                h = b.at[pl.ds(2 * i, 2)]
                send(h, h, qsend.at[s, zrel, 2 + i], qin_sem.at[s, zrel, 2 + i], dev(s, ps[s], qs[s] + (1 if i == 0 else 3), z, c))
                send(b, b, csend.at[s, zrel, 1 + i], cin_sem.at[s, zrel, 1 + i], dev(s, ps[s], qs[s], z, 1 - c))

    def far(zrel):
        for s in (0, 1):
            b = bundle(s, 2, zrel)
            for i in (0, 1):
                arrived(b.at[pl.ds(2 * i, 2)], qin_sem.at[s, zrel, 2 + i])
            send(b, b, csend.at[s, zrel, 3], cin_sem.at[s, zrel, 3], dev(s, ps[s], qs[s], z, 1 - c))

    column(1)
    column(7)
    ready(0)
    column(2)
    column(6)
    column(3)
    column(5)
    column(4)
    ready(1)
    ready(7)
    side(0)
    ready(2)
    ready(6)
    side(1)
    side(7)
    far(0)
    ready(3)
    ready(5)
    side(2)
    side(6)
    far(1)
    far(7)
    ready(4)
    side(3)
    side(5)
    far(2)
    far(6)
    side(4)
    far(3)
    far(5)
    far(4)
    for s in (0, 1):
        for zrel in (0, 1, 7, 2, 6, 3, 5, 4):
            for k, qrel in enumerate((0, 3, 1, 2)):
                qp = lax.rem(qs[1 - s] + qrel, 4)
                arrived(refs[s].at[1 - c, qp, zat(zrel)], cin_sem.at[s, zrel, k])
    for cp in sends:
        cp.wait_send()

def gather_nodes(own, out_space=pltpu.VMEM):
    dma = pltpu.SemaphoreType.DMA
    return pl.pallas_call(
        gather_kernel,
        out_shape=[jax.ShapeDtypeStruct((2, NR, NZ, NR, 24, 128), jnp.float32),
                   jax.ShapeDtypeStruct((2, NR, NZ, NR, 16, 128), jnp.float32)],
        in_specs=[pl.BlockSpec(memory_space=pltpu.VMEM)],
        out_specs=[pl.BlockSpec(memory_space=out_space)] * 2,
        scratch_shapes=[dma((2, 8, 3)), dma((2, 8)), dma((2, 8, 4)), dma((2, 8, 4)),
                        dma((2, 8, 3)), dma((2, 8)), dma((2, 8, 4)), dma((2, 8, 4)), dma((2,))],
        compiler_params=pltpu.CompilerParams(collective_id=0, has_side_effects=True, vmem_limit_bytes=40 << 20),
        name="gather_nodes",
    )(own)


F32 = jnp.float32
BF16 = jnp.bfloat16
TILE = 128
TILES = 16
LIST = 16
WIDE = 2
TOP = (0.053533121, 0.441039724, 1.53290974, 2.51582573, 3.00002466)
BOTTOM = (0.0316211711, 0.260817705, 0.838662982)
ROOT_PI = math.sqrt(math.pi)
K1 = 0.5 / ROOT_PI
K2_FIFTH = 0.25 / ROOT_PI / 5.0
EXP_RATE = -0.25 * math.log2(math.e)

def thirds(v):
    a = v.astype(BF16)
    r = v - a.astype(F32)
    b = r.astype(BF16)
    return a, b, (r - b.astype(F32)).astype(BF16)

def halves(v):
    a = v.astype(BF16)
    return a, (v - a.astype(F32)).astype(BF16)

def particle_rows(pos):
    x = pos[0:1] - 2.0
    y = pos[1:2] - 2.0
    z = pos[2:3] - 2.0
    none = jnp.zeros_like(x)
    xx, yy, zz = x * x, y * y, z * z
    dist = [-2.0 * x, -2.0 * y, -2.0 * z, none + 1.0, xx + yy + zz] + [none] * 11
    quad = [none] * 5 + [5.0 * x, 5.0 * y, 5.0 * z, none - 2.5, -2.5 * (xx - zz), -2.5 * (yy - zz), -5.0 * zz,
            -5.0 * (x * y), -5.0 * (x * z), -5.0 * (y * z), none]
    return jnp.concatenate(dist + quad, axis=0)

def node_rows(v):
    mass = v[0]
    x, y, z = v[1] - 2.0, v[2] - 2.0, v[3] - 2.0
    qxx, qyy, qzz, qxy, qxz, qyz = v[4:]
    qcx = qxx * x + qxy * y + qxz * z
    qcy = qxy * x + qyy * y + qyz * z
    qcz = qxz * x + qyz * y + qzz * z
    return [x, y, z, x * x + y * y + z * z + 0.25, jnp.ones_like(x), qcx, qcy, qcz,
            x * qcx + y * qcy + z * qcz, qxx, qyy, 0.5 * (qxx + qyy + qzz), qxy, qxz, qyz, (-1.0 / 3.0) * mass]

def force_kernel(counts_hbm, lists_hbm, pos_hbm, slot_hbm, v3, v2, out_ref,
                 nodes, rows_p, slot16, slot_col, feats, where_p, left, sb, cols, rb, total, forces, pos_ref, slot_ref, counts, lists, sems):
    fetch = [pltpu.make_async_copy(pos_hbm, pos_ref, sems.at[0]), pltpu.make_async_copy(slot_hbm, slot_ref, sems.at[1]),
             pltpu.make_async_copy(counts_hbm, counts, sems.at[2]), pltpu.make_async_copy(lists_hbm, lists, sems.at[3])]
    for cp in fetch:
        cp.start()
    lane = lax.broadcasted_iota(jnp.int32, (128, 128), 1)
    def node_step(i, _):
        u = 2 * i
        w = (u & 128) | ((u & 3) << 5) | (u & 28) | ((u >> 5) & 3)
        vals = []
        for k in range(10):
            if k < 6:
                a, b = v3[u, 4 * k:4 * k + 4, :], v3[u + 1, 4 * k:4 * k + 4, :]
            else:
                a, b = v2[w, 4 * k - 24:4 * k - 20, :], v2[w + 32, 4 * k - 24:4 * k - 20, :]
            vals.append(jnp.concatenate([a, b], axis=0))
        base = pl.multiple_of(i * 128, 128)
        for f, row in enumerate(node_rows(vals)):
            nodes[pl.ds(base + f, 8, stride=16), :] = row
        return 0
    lax.fori_loop(0, 128, node_step, 0, unroll=2)
    for cp in fetch:
        cp.wait()
    for r in range(16):
        slot16[r:r + 1, :] = slot_ref[0:1, r * 128:(r + 1) * 128]
    slot_t = slot16[...].T
    for r in range(16):
        slot_col[r] = jnp.broadcast_to(slot_t[:, r:r + 1], (128, 128))
    for i, piece in enumerate(thirds(particle_rows(pos_ref[...]))):
        rows_p[i * 32:(i + 1) * 32, :] = piece
    def tile_step(t, _):
        base = lane + t * 128
        acc = jnp.zeros((96, 128), F32)
        for r in range(0, 16, 2):
            hot = jnp.concatenate([(slot_col[r + h] == base).astype(F32).astype(BF16) for h in (0, 1)], axis=0)
            acc = acc + jnp.dot(rows_p[:, r * 128:(r + 2) * 128], hot, preferred_element_type=F32)
        got = acc.astype(BF16)
        for g, piece in enumerate((0, 0, 0, 1, 1, 2)):
            feats[t, g * 16:(g + 1) * 16, 0:128] = got[piece * 32:piece * 32 + 16]
            feats[t, g * 16:(g + 1) * 16, 128:256] = got[piece * 32 + 16:piece * 32 + 32]
        where_p[t] = -0.5 * (acc[0:8] + acc[32:40] + acc[64:72])
        return 0
    lax.fori_loop(0, TILES, tile_step, 0)
    total[...] = jnp.zeros_like(total)
    def block_row(b):
        d = b >> 2
        c, z = d & 1, (d >> 1) & 7
        x, y = ((d >> 3) & 2) | ((d >> 7) & 1), (d >> 5) & 3
        p = jnp.where(c == 0, x, y)
        q = jnp.where(c == 0, y, x)
        return ((((c * 4 + q) * 8 + z) * 4 + p) * 4 + (b & 3)) * 16

    live = lax.fori_loop(0, TILES, lambda t, n: n + counts[t], 0)

    def take(t, k):
        ok = t < TILES
        at = jnp.minimum(t, TILES - 1)
        row = block_row(jnp.where(ok, lists[at, k], 0))
        last = k + 1 >= counts[at]
        return (row, t), (jnp.where(ok & last, t + 1, t), jnp.where(last, 0, k + 1))

    def node_at(row):
        return nodes[pl.ds(pl.multiple_of(row, 16), 16), :]

    def sums(h, pair):
        row, t = pair
        hi, lo = halves(node_at(row))
        both = jnp.concatenate([jnp.concatenate([hi, hi], axis=1), jnp.concatenate([lo, lo], axis=1)], axis=0)
        return jnp.dot(both, rb[h], preferred_element_type=F32)

    def radial(h):
        for r in range(0, 128, 16):
            s2 = sb[h, r:r + 16, 0:128]
            inner = sb[h, r:r + 16, 128:256]
            mass = jnp.broadcast_to(cols[h, r:r + 16, 15:16], (16, 128))
            trace = jnp.broadcast_to(cols[h, r:r + 16, 11:12], (16, 128))
            w = lax.rsqrt(s2)
            e = jnp.exp2(s2 * EXP_RATE)
            top = TOP[4] * w + TOP[3]
            for coef in TOP[2::-1]:
                top = top * w + coef
            bottom = w + BOTTOM[2]
            for coef in BOTTOM[1::-1]:
                bottom = bottom * w + coef
            u = w * w
            a1 = top * pl.reciprocal(bottom) * u
            g2 = (a1 + K1) * u
            g3 = (g2 + K2_FIFTH) * u
            hi, lo = halves(e * (mass * a1 + trace * g2 + inner * g3))
            rb[h, r:r + 16, 0:128] = hi
            rb[h, 128 + r:128 + r + 16, 0:128] = lo
            hi, lo = halves(e * g2)
            rb[h, r:r + 16, 128:256] = hi
            rb[h, 128 + r:128 + r + 16, 128:256] = lo

    def products(h, pair):
        row, t = pair
        sb[h] = jnp.dot(left[h], feats[jnp.minimum(t, TILES - 1)], preferred_element_type=F32)
        cols[h, :, 0:16] = node_at(row).T

    def prepare(h, pair):
        p1, p2, p3 = thirds(node_at(pair[0]))
        left[h] = jnp.concatenate([p1, p2, p3, p1, p2, p1], axis=0).T

    idle = ((0, TILES),) * WIDE

    def pair_step(i, carry):
        at, first, second, third, fourth = carry
        got = [sums(h, fourth[h]) for h in range(WIDE)]
        for h in range(WIDE):
            radial(h)
        for h in range(WIDE):
            products(h, second[h])
        for h in range(WIDE):
            prepare(h, first[h])
        for h in range(WIDE):
            total[fourth[h][1]] += got[h]
        fresh = []
        for h in range(WIDE):
            pair, at = take(*at)
            fresh.append(pair)
        return at, tuple(fresh), first, second, third
    at = (0, 0)
    begin = []
    for h in range(WIDE):
        pair, at = take(*at)
        begin.append(pair)
    lax.fori_loop(0, (live + WIDE - 1) // WIDE + 3, pair_step, (at, tuple(begin), idle, idle, idle))

    for t in range(TILES):
        s = total[t, 0:16, :] + total[t, 16:32, :]
        x, y, z = where_p[t, 0:1, :], where_p[t, 1:2, :], where_p[t, 2:3, :]
        rad = lambda k: s[k:k + 1, 0:128]
        sec = lambda k: s[k:k + 1, 128:256]
        m = rad(4)
        xx, yy, xy, xz, yz = sec(9), sec(10), sec(12), sec(13), sec(14)
        zz = 2.0 * sec(11) - xx - yy
        forces[0, t:t + 1, :] = x * m - rad(0) + xx * x + xy * y + xz * z - sec(5)
        forces[1, t:t + 1, :] = y * m - rad(1) + xy * x + yy * y + yz * z - sec(6)
        forces[2, t:t + 1, :] = z * m - rad(2) + xz * x + yz * y + zz * z - sec(7)
    slot = slot16[...]
    at = slot % 128
    tile = slot // 128
    for k in range(3):
        got = jnp.zeros((16, 128), F32)
        for t in range(TILES):
            row = jnp.broadcast_to(forces[k, t:t + 1, :], (16, 128))
            got = jnp.where(tile == t, jnp.take_along_axis(row, at, axis=1), got)
        for r in range(16):
            out_ref[k:k + 1, r * 128:(r + 1) * 128] = got[r:r + 1, :]

def forces_of(counts, lists, pos, slots, v3, v2):
    vmem = pl.BlockSpec(memory_space=pltpu.VMEM)
    hbm = pl.BlockSpec(memory_space=pltpu.HBM)
    return pl.pallas_call(
        force_kernel,
        out_shape=jax.ShapeDtypeStruct(pos.shape, F32),
        in_specs=[hbm, hbm, hbm, hbm, vmem, vmem],
        out_specs=vmem,
        scratch_shapes=[pltpu.VMEM((1024 * 16, 128), F32), pltpu.VMEM((96, 2048), BF16), pltpu.VMEM((16, 128), jnp.int32),
                        pltpu.VMEM((16, 128, 128), jnp.int32), pltpu.VMEM((16, 96, 256), BF16), pltpu.VMEM((16, 8, 128), F32),
                        pltpu.VMEM((WIDE, 128, 96), BF16), pltpu.VMEM((WIDE, 128, 256), F32), pltpu.VMEM((WIDE, 128, 128), F32),
                        pltpu.VMEM((WIDE, 256, 256), BF16), pltpu.VMEM((17, 32, 256), F32), pltpu.VMEM((3, 16, 128), F32),
                        pltpu.VMEM((3, 2048), F32), pltpu.VMEM((1, 2048), jnp.int32), pltpu.SMEM((16,), jnp.int32), pltpu.SMEM((16, 16), jnp.int32), pltpu.SemaphoreType.DMA((4,))],
        compiler_params=pltpu.CompilerParams(vmem_limit_bytes=24 << 20),
        name="tile_forces",
    )(*(pltpu.with_memory_space_constraint(a, pltpu.HBM) for a in (counts, lists, pos, slots)), v3.reshape(256, 24, 128), v2.reshape(256, 16, 128))


def shards(positions, node_moments, slot_of, block_list, tile_counts):
    own = node_moments.reshape(40, 128)
    v3, v2 = gather_nodes(own)
    return forces_of(tile_counts, block_list, positions, slot_of, v3, v2)


def solution(mesh):
    placed = (
        P(None, ("gx", "gy")),
        P(None, ("gx", "gy")),
        P(("gx", "gy"), None),
        P(("gx", "gy"), None),
        P(("gx", "gy")),
    )
    return jax.shard_map(
        shards, mesh=mesh, in_specs=placed, out_specs=P(None, ("gx", "gy")), check_vma=False
    )
```

```python
import functools
import math

import jax
import jax.numpy as jnp
from jax import lax
from jax.experimental import pallas as pl
from jax.experimental.pallas import tpu as pltpu
from jax.sharding import PartitionSpec as P

F32 = jnp.float32
BF16 = jnp.bfloat16
TILE = 128
TILES = 16
MESH = pl.DeviceIdType.MESH
NZ = 8
NR = 4

def thirds(v):
    a = v.astype(BF16)
    r = v - a.astype(F32)
    b = r.astype(BF16)
    return a, b, (r - b.astype(F32)).astype(BF16)

def particle_rows(pos):
    x = pos[0:1] - 2.0
    y = pos[1:2] - 2.0
    z = pos[2:3] - 2.0
    none = jnp.zeros_like(x)
    xx, yy, zz = x * x, y * y, z * z
    dist = [-2.0 * x, -2.0 * y, -2.0 * z, none + 1.0, xx + yy + zz] + [none] * 11
    quad = [none] * 5 + [5.0 * x, 5.0 * y, 5.0 * z, none - 2.5, -2.5 * (xx - zz), -2.5 * (yy - zz), -5.0 * zz,
            -5.0 * (x * y), -5.0 * (x * z), -5.0 * (y * z), none]
    return jnp.concatenate(dist + quad, axis=0)

def node_rows(v):
    mass = v[0]
    x, y, z = v[1] - 2.0, v[2] - 2.0, v[3] - 2.0
    qxx, qyy, qzz, qxy, qxz, qyz = v[4:]
    qcx = qxx * x + qxy * y + qxz * z
    qcy = qxy * x + qyy * y + qyz * z
    qcz = qxz * x + qyz * y + qzz * z
    return [x, y, z, x * x + y * y + z * z + 0.25, jnp.ones_like(x), qcx, qcy, qcz,
            x * qcx + y * qcy + z * qcz, qxx, qyy, 0.5 * (qxx + qyy + qzz), qxy, qxz, qyz, (-1.0 / 3.0) * mass]

def device_of(first, p, q, z, c):
    x = first * p + (1 - first) * q
    y = first * q + (1 - first) * p
    return (lax.rem(x, 2) * 4 + y, (x // 2) * 16 + z * 2 + c)

ZPOS = (0, 1, 3, 5, 7, 6, 4, 2)
GROUPS = ((0, 1), (1, 5), (5, 8))
P_STEPS = ((0, 1), (1, 3), (2, 2))
Z_STEPS = (1, 7, 2, 6, 3, 5, 4)

def gather_kernel(nodes_hbm, pos_hbm, slot_hbm, nodes, feats, where_p, slot16,
                  v3, v2, own_ref, pos_ref, slot_ref, rows_p, slot_col, stage, load_sem, pin_sem, zin_sem, qin_sem, cin_sem, psend, zsend, qsend, csend, own_sem):
    gx = lax.axis_index("gx")
    gy = lax.axis_index("gy")
    c = lax.rem(gy, 2)
    z = lax.rem(gy // 2, 8)
    x = (gy // 16) * 2 + gx // 4
    y = lax.rem(gx, 4)
    refs = (v3, v2)
    rows = ((0, 24), (24, 16))
    firsts = (1 - c, c)
    ps = tuple(f * x + (1 - f) * y for f in firsts)
    qs = tuple(f * y + (1 - f) * x for f in firsts)

    def dev(s, p, q, zz, cc):
        return device_of(firsts[s], lax.rem(p, 4), lax.rem(q, 4), lax.rem(zz, 8), cc)

    def qat(s, rel):
        return lax.rem(qs[s] + rel, 4)

    def span(g):
        lo, hi = GROUPS[g]
        return pl.ds(lo, hi - lo)

    for q in range(10):
        for b in range(4):
            pltpu.make_async_copy(nodes_hbm.at[pl.ds(q, 1), pl.ds(b * 128, 128)], own_ref.at[pl.ds(q * 4 + b, 1)], load_sem.at[0]).start()
    fetch = [pltpu.make_async_copy(pos_hbm, pos_ref, load_sem.at[1]), pltpu.make_async_copy(slot_hbm, slot_ref, load_sem.at[2])]
    for cp in fetch:
        cp.start()

    barrier = pltpu.get_barrier_semaphore()
    peers = [device_of(1, x, y, z, 1 - c)]
    for d in (1, 2, 3):
        peers.append(device_of(1, lax.rem(x + d, 4), y, z, c))
        peers.append(device_of(1, x, lax.rem(y + d, 4), z, c))
    for d in range(1, 8):
        peers.append(device_of(1, x, y, lax.rem(z + d, 8), c))
    for peer in peers:
        pl.semaphore_signal(barrier, inc=1, device_id=peer, device_id_type=MESH)
    pltpu.make_async_copy(own_ref, own_ref, load_sem.at[0]).wait()
    pl.semaphore_wait(barrier, len(peers))

    sends = []

    def send(src, dst, ssem, rsem, to):
        cp = pltpu.make_async_remote_copy(src_ref=src, dst_ref=dst, send_sem=ssem, recv_sem=rsem, device_id=to, device_id_type=MESH)
        cp.start()
        sends.append(cp)

    def arrived(ref, sem):
        pltpu.make_async_remote_copy(src_ref=ref, dst_ref=ref, send_sem=sem, recv_sem=sem, device_id=(gx, gy), device_id_type=MESH).wait_recv()

    for d in Z_STEPS:
        pos = ZPOS[8 - d]
        send(own_ref, stage.at[pos], zsend.at[pos], zin_sem.at[pos], dev(0, ps[0], qs[0], z + d, c))
    local = {}

    def column(g):
        lo, hi = GROUPS[g]
        for pos in range(max(lo, 1), hi):
            arrived(stage.at[pos], zin_sem.at[pos])
        for s in (0, 1):
            r0, rn = rows[s]
            src = own_ref.at[pl.ds(r0, rn)] if hi == 1 else stage.at[span(g), pl.ds(r0, rn)]
            at = 0 if hi == 1 else span(g)
            dst = refs[s].at[c, qs[s], at, ps[s]]
            for i, d in P_STEPS:
                send(src, dst, psend.at[s, g, i], pin_sem.at[s, g, i], dev(s, ps[s] + d, qs[s], z, c))
            cp = pltpu.make_async_copy(src, dst, own_sem.at[s, g])
            cp.start()
            local[s, g] = cp

    def bundle(s, qrel, g):
        return refs[s].at[c, qat(s, qrel), span(g)]

    def ready(g):
        lo, hi = GROUPS[g]
        for s in (0, 1):
            for i, d in P_STEPS:
                at = 0 if hi == 1 else span(g)
                arrived(refs[s].at[c, qs[s], at, lax.rem(ps[s] + 4 - d, 4)], pin_sem.at[s, g, i])
            local[s, g].wait()
            b = bundle(s, 0, g)
            send(b, b, qsend.at[s, g, 0], qin_sem.at[s, g, 0], dev(s, ps[s], qs[s] + 1, z, c))
            send(b, b, qsend.at[s, g, 1], qin_sem.at[s, g, 1], dev(s, ps[s], qs[s] + 3, z, c))
            send(b, b, csend.at[s, g, 0], cin_sem.at[s, g, 0], dev(s, ps[s], qs[s], z, 1 - c))

    def side(g):
        for s in (0, 1):
            for i, rel in ((0, 3), (1, 1)):
                b = bundle(s, rel, g)
                arrived(b, qin_sem.at[s, g, i])
                h = refs[s].at[c, qat(s, rel), span(g), pl.ds(2 * i, 2)]
                send(h, h, qsend.at[s, g, 2 + i], qin_sem.at[s, g, 2 + i], dev(s, ps[s], qs[s] + (1 if i == 0 else 3), z, c))
                send(b, b, csend.at[s, g, 1 + i], cin_sem.at[s, g, 1 + i], dev(s, ps[s], qs[s], z, 1 - c))

    def far(g):
        for s in (0, 1):
            for i in (0, 1):
                arrived(refs[s].at[c, qat(s, 2), span(g), pl.ds(2 * i, 2)], qin_sem.at[s, g, 2 + i])
            b = bundle(s, 2, g)
            send(b, b, csend.at[s, g, 3], cin_sem.at[s, g, 3], dev(s, ps[s], qs[s], z, 1 - c))

    tiles_done = [0]

    def particle_prep():
        for cp in fetch:
            cp.wait()
        for r in range(16):
            slot16[r:r + 1, :] = slot_ref[0:1, r * 128:(r + 1) * 128]
        slot_t = slot16[...].T
        for r in range(16):
            slot_col[r] = jnp.broadcast_to(slot_t[:, r:r + 1], (128, 128))
        for i, piece in enumerate(thirds(particle_rows(pos_ref[...]))):
            rows_p[i * 32:(i + 1) * 32, :] = piece

    lane = lax.broadcasted_iota(jnp.int32, (128, 128), 1)

    def tile_step(t, _):
        base = lane + t * 128
        acc = jnp.zeros((96, 128), F32)
        for r in range(0, 16, 2):
            hot = jnp.concatenate([(slot_col[r + h] == base).astype(F32).astype(BF16) for h in (0, 1)], axis=0)
            acc = acc + jnp.dot(rows_p[:, r * 128:(r + 2) * 128], hot, preferred_element_type=F32)
        got = acc.astype(BF16)
        for g, piece in enumerate((0, 0, 0, 1, 1, 2)):
            feats[t, g * 16:(g + 1) * 16, 0:128] = got[piece * 32:piece * 32 + 16]
            feats[t, g * 16:(g + 1) * 16, 128:256] = got[piece * 32 + 16:piece * 32 + 32]
        where_p[t] = -0.5 * (acc[0:8] + acc[32:40] + acc[64:72])
        return 0

    def particle_tiles(n):
        lax.fori_loop(tiles_done[0], tiles_done[0] + n, tile_step, 0)
        tiles_done[0] += n

    def partner(g):
        for s in (0, 1):
            for k, qrel in enumerate((0, 3, 1, 2)):
                qp = lax.rem(qs[1 - s] + qrel, 4)
                arrived(refs[s].at[1 - c, qp, span(g)], cin_sem.at[s, g, k])

    def features(core, g):
        lo, hi = GROUPS[g]

        def step(j, _):
            at = lo + j
            for q in range(4):
                for p in (0, 2):
                    vals = []
                    for k in range(10):
                        if k < 6:
                            a, b = v3[core, q, at, p, 4 * k:4 * k + 4, :], v3[core, q, at, p + 1, 4 * k:4 * k + 4, :]
                        else:
                            r = 4 * k - 24
                            a, b = v2[core, p, at, q, r:r + 4, :], v2[core, p + 1, at, q, r:r + 4, :]
                        vals.append(jnp.concatenate([a, b], axis=0))
                    base = pl.multiple_of(((core * 4 + q) * 8 + at) * 256 + p * 64, 128)
                    for f, row in enumerate(node_rows(vals)):
                        nodes[pl.ds(base + f, 8, stride=16), :] = row
            return 0
        lax.fori_loop(0, hi - lo, step, 0)

    particle_prep()
    column(0)
    particle_tiles(2)
    column(1)
    particle_tiles(2)
    column(2)
    particle_tiles(2)
    ready(0)
    particle_tiles(3)
    ready(1)
    particle_tiles(3)
    ready(2)
    particle_tiles(4)
    side(0)
    side(1)
    side(2)
    far(0)
    features(c, 0)
    far(1)
    far(2)
    features(c, 1)
    partner(0)
    features(1 - c, 0)
    partner(1)
    features(1 - c, 1)
    features(c, 2)
    partner(2)
    features(1 - c, 2)
    for cp in sends:
        cp.wait_send()

def gather_nodes(nodes, pos, slots):
    dma = pltpu.SemaphoreType.DMA
    n = len(GROUPS)
    vmem = pl.BlockSpec(memory_space=pltpu.VMEM)
    hbm = pl.BlockSpec(memory_space=pltpu.HBM)
    return pl.pallas_call(
        gather_kernel,
        out_shape=[jax.ShapeDtypeStruct((1024 * 16, 128), F32),
                   jax.ShapeDtypeStruct((TILES, 96, 256), BF16),
                   jax.ShapeDtypeStruct((TILES, 8, 128), F32),
                   jax.ShapeDtypeStruct((16, 128), jnp.int32)],
        in_specs=[hbm] * 3,
        out_specs=[vmem] * 4,
        scratch_shapes=[pltpu.VMEM((2, NR, NZ, NR, 24, 128), F32), pltpu.VMEM((2, NR, NZ, NR, 16, 128), F32),
                        pltpu.VMEM((40, 128), F32), pltpu.VMEM((3, 2048), F32), pltpu.VMEM((1, 2048), jnp.int32),
                        pltpu.VMEM((96, 2048), BF16), pltpu.VMEM((16, 128, 128), jnp.int32),
                        pltpu.VMEM((8, 40, 128), F32), dma((3,)),
                        dma((2, n, 3)), dma((8,)), dma((2, n, 4)), dma((2, n, 4)),
                        dma((2, n, 3)), dma((8,)), dma((2, n, 4)), dma((2, n, 4)), dma((2, n))],
        compiler_params=pltpu.CompilerParams(collective_id=0, has_side_effects=True, vmem_limit_bytes=20 << 20),
        name="gather_nodes",
    )(*(pltpu.with_memory_space_constraint(a, pltpu.HBM) for a in (nodes, pos, slots)))


WIDE = 2
TOP = (0.053533121, 0.441039724, 1.53290974, 2.51582573, 3.00002466)
BOTTOM = (0.0316211711, 0.260817705, 0.838662982)
ROOT_PI = math.sqrt(math.pi)
K1 = 0.5 / ROOT_PI
K2_FIFTH = 0.25 / ROOT_PI / 5.0
EXP_RATE = -0.25 * math.log2(math.e)

def halves(v):
    a = v.astype(BF16)
    return a, (v - a.astype(F32)).astype(BF16)

def force_kernel(counts_hbm, lists_hbm, nodes, feats, where_p, slot16, out_ref, left, sb, cols, rb, total, forces, counts, lists, sems):
    fetch = [pltpu.make_async_copy(counts_hbm, counts, sems.at[0]), pltpu.make_async_copy(lists_hbm, lists, sems.at[1])]
    for cp in fetch:
        cp.start()
    own_z = (lax.axis_index("gy") >> 1) & 7
    for cp in fetch:
        cp.wait()
    total[...] = jnp.zeros_like(total)
    def block_row(b):
        d = b >> 2
        c, z = d & 1, ((d >> 1) - own_z) & 7
        z = jnp.where(z > 4, 16 - 2 * z, jnp.maximum(2 * z - 1, 0))
        x, y = ((d >> 3) & 2) | ((d >> 7) & 1), (d >> 5) & 3
        p = jnp.where(c == 0, x, y)
        q = jnp.where(c == 0, y, x)
        return ((((c * 4 + q) * 8 + z) * 4 + p) * 4 + (b & 3)) * 16

    live = lax.fori_loop(0, TILES, lambda t, n: n + counts[t], 0)

    def take(t, k):
        ok = t < TILES
        at = jnp.minimum(t, TILES - 1)
        row = block_row(jnp.where(ok, lists[at, k], 0))
        last = k + 1 >= counts[at]
        return (row, t), (jnp.where(ok & last, t + 1, t), jnp.where(last, 0, k + 1))

    def node_at(row):
        return nodes[pl.ds(pl.multiple_of(row, 16), 16), :]

    def sums(h, pair):
        row, t = pair
        hi, lo = halves(node_at(row))
        both = jnp.concatenate([jnp.concatenate([hi, hi], axis=1), jnp.concatenate([lo, lo], axis=1)], axis=0)
        return jnp.dot(both, rb[h], preferred_element_type=F32)

    def radial(h):
        for r in range(0, 128, 16):
            s2 = sb[h, r:r + 16, 0:128]
            inner = sb[h, r:r + 16, 128:256]
            mass = jnp.broadcast_to(cols[h, r:r + 16, 15:16], (16, 128))
            trace = jnp.broadcast_to(cols[h, r:r + 16, 11:12], (16, 128))
            w = lax.rsqrt(s2)
            e = jnp.exp2(s2 * EXP_RATE)
            top = TOP[4] * w + TOP[3]
            for coef in TOP[2::-1]:
                top = top * w + coef
            bottom = w + BOTTOM[2]
            for coef in BOTTOM[1::-1]:
                bottom = bottom * w + coef
            u = w * w
            a1 = top * pl.reciprocal(bottom) * u
            g2 = (a1 + K1) * u
            g3 = (g2 + K2_FIFTH) * u
            hi, lo = halves(e * (mass * a1 + trace * g2 + inner * g3))
            rb[h, r:r + 16, 0:128] = hi
            rb[h, 128 + r:128 + r + 16, 0:128] = lo
            hi, lo = halves(e * g2)
            rb[h, r:r + 16, 128:256] = hi
            rb[h, 128 + r:128 + r + 16, 128:256] = lo

    def products(h, pair):
        row, t = pair
        sb[h] = jnp.dot(left[h], feats[jnp.minimum(t, TILES - 1)], preferred_element_type=F32)
        cols[h, :, 0:16] = node_at(row).T

    def prepare(h, pair):
        p1, p2, p3 = thirds(node_at(pair[0]))
        left[h] = jnp.concatenate([p1, p2, p3, p1, p2, p1], axis=0).T

    idle = ((0, TILES),) * WIDE

    def pair_step(i, carry):
        at, first, second, third, fourth = carry
        got = [sums(h, fourth[h]) for h in range(WIDE)]
        for h in range(WIDE):
            radial(h)
        for h in range(WIDE):
            products(h, second[h])
        for h in range(WIDE):
            prepare(h, first[h])
        for h in range(WIDE):
            total[fourth[h][1]] += got[h]
        fresh = []
        for h in range(WIDE):
            pair, at = take(*at)
            fresh.append(pair)
        return at, tuple(fresh), first, second, third
    at = (0, 0)
    begin = []
    for h in range(WIDE):
        pair, at = take(*at)
        begin.append(pair)
    lax.fori_loop(0, (live + WIDE - 1) // WIDE + 3, pair_step, (at, tuple(begin), idle, idle, idle))

    for t in range(TILES):
        s = total[t, 0:16, :] + total[t, 16:32, :]
        x, y, z = where_p[t, 0:1, :], where_p[t, 1:2, :], where_p[t, 2:3, :]
        rad = lambda k: s[k:k + 1, 0:128]
        sec = lambda k: s[k:k + 1, 128:256]
        m = rad(4)
        xx, yy, xy, xz, yz = sec(9), sec(10), sec(12), sec(13), sec(14)
        zz = 2.0 * sec(11) - xx - yy
        forces[0, t:t + 1, :] = x * m - rad(0) + xx * x + xy * y + xz * z - sec(5)
        forces[1, t:t + 1, :] = y * m - rad(1) + xy * x + yy * y + yz * z - sec(6)
        forces[2, t:t + 1, :] = z * m - rad(2) + xz * x + yz * y + zz * z - sec(7)
    slot = slot16[...]
    at = slot % 128
    tile = slot // 128
    for k in range(3):
        got = jnp.zeros((16, 128), F32)
        for t in range(TILES):
            row = jnp.broadcast_to(forces[k, t:t + 1, :], (16, 128))
            got = jnp.where(tile == t, jnp.take_along_axis(row, at, axis=1), got)
        for r in range(16):
            out_ref[k:k + 1, r * 128:(r + 1) * 128] = got[r:r + 1, :]

def forces_of(counts, lists, nodes, feats, where_p, slots):
    vmem = pl.BlockSpec(memory_space=pltpu.VMEM)
    hbm = pl.BlockSpec(memory_space=pltpu.HBM)
    return pl.pallas_call(
        force_kernel,
        out_shape=jax.ShapeDtypeStruct((3, TILES * TILE), F32),
        in_specs=[hbm, hbm, vmem, vmem, vmem, vmem],
        out_specs=vmem,
        scratch_shapes=[pltpu.VMEM((WIDE, 128, 96), BF16), pltpu.VMEM((WIDE, 128, 256), F32), pltpu.VMEM((WIDE, 128, 128), F32),
                        pltpu.VMEM((WIDE, 256, 256), BF16), pltpu.VMEM((17, 32, 256), F32), pltpu.VMEM((3, 16, 128), F32),
                        pltpu.SMEM((16,), jnp.int32), pltpu.SMEM((16, 16), jnp.int32), pltpu.SemaphoreType.DMA((2,))],
        compiler_params=pltpu.CompilerParams(vmem_limit_bytes=16 << 20),
        name="tile_forces",
    )(*(pltpu.with_memory_space_constraint(a, pltpu.HBM) for a in (counts, lists)), nodes, feats, where_p, slots)


def shards(positions, node_moments, slot_of, block_list, tile_counts):
    nodes, feats, where_p, slots = gather_nodes(node_moments, positions, slot_of)
    return forces_of(tile_counts, block_list, nodes, feats, where_p, slots)


def solution(mesh):
    placed = (
        P(None, ("gx", "gy")),
        P(None, ("gx", "gy")),
        P(("gx", "gy"), None),
        P(("gx", "gy"), None),
        P(("gx", "gy")),
    )
    return jax.shard_map(
        shards, mesh=mesh, in_specs=placed, out_specs=P(None, ("gx", "gy")), check_vma=False
    )
```

```python
import functools
import math

import jax
import jax.numpy as jnp
from jax import lax
from jax.experimental import pallas as pl
from jax.experimental.pallas import tpu as pltpu
from jax.sharding import PartitionSpec as P

F32 = jnp.float32
BF16 = jnp.bfloat16
TILE = 128
TILES = 16
RATE = 0.25 * math.log2(math.e)
SCALE = 3.00002466 * math.sqrt(RATE)
TOP = (0.137173002, 0.67870502, 1.41669777, 1.3963634)
BOTTOM = (0.145984292, 0.723140227, 1.39646547)
ROOT_PI = math.sqrt(math.pi)
FIRST = 0.5 / ROOT_PI / (SCALE * RATE)
SECOND = 0.05 / ROOT_PI / (SCALE * RATE**2)
MESH = pl.DeviceIdType.MESH
NZ = 8
NR = 4

def thirds(v):
    a = v.astype(BF16)
    r = v - a.astype(F32)
    b = r.astype(BF16)
    return a, b, (r - b.astype(F32)).astype(BF16)

def particle_rows(pos):
    x = pos[0:1] - 2.0
    y = pos[1:2] - 2.0
    z = pos[2:3] - 2.0
    none = jnp.zeros_like(x)
    xx, yy, zz = x * x, y * y, z * z
    g = -2.5 * SCALE * RATE**3
    dist = [-2.0 * RATE * x, -2.0 * RATE * y, -2.0 * RATE * z, none + RATE, RATE * (xx + yy + zz)] + [none] * 11
    quad = [none] * 5 + [-2.0 * g * x, -2.0 * g * y, -2.0 * g * z, none + g, g * (xx - zz), g * (yy - zz), -5.0 * RATE * zz,
            2.0 * g * (x * y), 2.0 * g * (x * z), 2.0 * g * (y * z), none]
    return jnp.concatenate(dist + quad, axis=0)

def node_rows(v):
    mass = v[0]
    x, y, z = v[1] - 2.0, v[2] - 2.0, v[3] - 2.0
    qxx, qyy, qzz, qxy, qxz, qyz = v[4:]
    qcx = qxx * x + qxy * y + qxz * z
    qcy = qxy * x + qyy * y + qyz * z
    qcz = qxz * x + qyz * y + qzz * z
    return [x, y, z, x * x + y * y + z * z + 0.25, jnp.ones_like(x), qcx, qcy, qcz,
            x * qcx + y * qcy + z * qcz, qxx, qyy, (0.5 * SCALE * RATE**2) * (qxx + qyy + qzz), qxy, qxz, qyz,
            (-SCALE * RATE / 3.0) * mass]

def device_of(first, p, q, z, c):
    x = first * p + (1 - first) * q
    y = first * q + (1 - first) * p
    return (lax.rem(x, 2) * 4 + y, (x // 2) * 16 + z * 2 + c)

ZPOS = (0, 1, 3, 5, 7, 6, 4, 2)
GROUPS = ((0, 1), (1, 5), (5, 8))
P_STEPS = ((0, 1), (1, 3), (2, 2))
Z_STEPS = (1, 7, 2, 6, 3, 5, 4)

def gather_kernel(nodes_hbm, pos_hbm, slot_hbm, counts_hbm, lists_hbm, nodes, feats, where_p, slot16, counts, lists,
                  v3, v2, own_ref, pos_ref, slot_ref, rows_p, slot_col, stage, load_sem, pin_sem, zin_sem, qin_sem, cin_sem, psend, zsend, qsend, csend, own_sem):
    gx = lax.axis_index("gx")
    gy = lax.axis_index("gy")
    c = lax.rem(gy, 2)
    z = lax.rem(gy // 2, 8)
    x = (gy // 16) * 2 + gx // 4
    y = lax.rem(gx, 4)
    refs = (v3, v2)
    rows = ((0, 24), (24, 16))
    firsts = (1 - c, c)
    ps = tuple(f * x + (1 - f) * y for f in firsts)
    qs = tuple(f * y + (1 - f) * x for f in firsts)

    def dev(s, p, q, zz, cc):
        return device_of(firsts[s], lax.rem(p, 4), lax.rem(q, 4), lax.rem(zz, 8), cc)

    def qat(s, rel):
        return lax.rem(qs[s] + rel, 4)

    def span(g):
        lo, hi = GROUPS[g]
        return pl.ds(lo, hi - lo)

    for q in range(10):
        for b in range(4):
            pltpu.make_async_copy(nodes_hbm.at[pl.ds(q, 1), pl.ds(b * 128, 128)], own_ref.at[pl.ds(q * 4 + b, 1)], load_sem.at[0]).start()
    fetch = [pltpu.make_async_copy(pos_hbm, pos_ref, load_sem.at[1]), pltpu.make_async_copy(slot_hbm, slot_ref, load_sem.at[2]),
             pltpu.make_async_copy(counts_hbm, counts, load_sem.at[3]), pltpu.make_async_copy(lists_hbm, lists, load_sem.at[4])]
    for cp in fetch:
        cp.start()

    barrier = pltpu.get_barrier_semaphore()
    peers = [device_of(1, x, y, z, 1 - c)]
    for d in (1, 2, 3):
        peers.append(device_of(1, lax.rem(x + d, 4), y, z, c))
        peers.append(device_of(1, x, lax.rem(y + d, 4), z, c))
    for d in range(1, 8):
        peers.append(device_of(1, x, y, lax.rem(z + d, 8), c))
    for peer in peers:
        pl.semaphore_signal(barrier, inc=1, device_id=peer, device_id_type=MESH)
    pltpu.make_async_copy(own_ref, own_ref, load_sem.at[0]).wait()
    pl.semaphore_wait(barrier, len(peers))

    sends = []

    def send(src, dst, ssem, rsem, to):
        cp = pltpu.make_async_remote_copy(src_ref=src, dst_ref=dst, send_sem=ssem, recv_sem=rsem, device_id=to, device_id_type=MESH)
        cp.start()
        sends.append(cp)

    def arrived(ref, sem):
        pltpu.make_async_remote_copy(src_ref=ref, dst_ref=ref, send_sem=sem, recv_sem=sem, device_id=(gx, gy), device_id_type=MESH).wait_recv()

    for d in Z_STEPS:
        pos = ZPOS[8 - d]
        send(own_ref, stage.at[pos], zsend.at[pos], zin_sem.at[pos], dev(0, ps[0], qs[0], z + d, c))
    local = {}

    def column(g):
        lo, hi = GROUPS[g]
        for pos in range(max(lo, 1), hi):
            arrived(stage.at[pos], zin_sem.at[pos])
        for s in (0, 1):
            r0, rn = rows[s]
            src = own_ref.at[pl.ds(r0, rn)] if hi == 1 else stage.at[span(g), pl.ds(r0, rn)]
            at = 0 if hi == 1 else span(g)
            dst = refs[s].at[c, qs[s], at, ps[s]]
            for i, d in P_STEPS:
                send(src, dst, psend.at[s, g, i], pin_sem.at[s, g, i], dev(s, ps[s] + d, qs[s], z, c))
            cp = pltpu.make_async_copy(src, dst, own_sem.at[s, g])
            cp.start()
            local[s, g] = cp

    def bundle(s, qrel, g):
        return refs[s].at[c, qat(s, qrel), span(g)]

    def ready(g):
        lo, hi = GROUPS[g]
        for s in (0, 1):
            for i, d in P_STEPS:
                at = 0 if hi == 1 else span(g)
                arrived(refs[s].at[c, qs[s], at, lax.rem(ps[s] + 4 - d, 4)], pin_sem.at[s, g, i])
            local[s, g].wait()
            b = bundle(s, 0, g)
            send(b, b, qsend.at[s, g, 0], qin_sem.at[s, g, 0], dev(s, ps[s], qs[s] + 1, z, c))
            send(b, b, qsend.at[s, g, 1], qin_sem.at[s, g, 1], dev(s, ps[s], qs[s] + 3, z, c))
            send(b, b, csend.at[s, g, 0], cin_sem.at[s, g, 0], dev(s, ps[s], qs[s], z, 1 - c))

    def side(g):
        for s in (0, 1):
            for i, rel in ((0, 3), (1, 1)):
                b = bundle(s, rel, g)
                arrived(b, qin_sem.at[s, g, i])
                h = refs[s].at[c, qat(s, rel), span(g), pl.ds(2 * i, 2)]
                send(h, h, qsend.at[s, g, 2 + i], qin_sem.at[s, g, 2 + i], dev(s, ps[s], qs[s] + (1 if i == 0 else 3), z, c))
                send(b, b, csend.at[s, g, 1 + i], cin_sem.at[s, g, 1 + i], dev(s, ps[s], qs[s], z, 1 - c))

    def far(g):
        for s in (0, 1):
            for i in (0, 1):
                arrived(refs[s].at[c, qat(s, 2), span(g), pl.ds(2 * i, 2)], qin_sem.at[s, g, 2 + i])
            b = bundle(s, 2, g)
            send(b, b, csend.at[s, g, 3], cin_sem.at[s, g, 3], dev(s, ps[s], qs[s], z, 1 - c))

    tiles_done = [0]

    def particle_prep():
        for cp in fetch:
            cp.wait()
        for r in range(16):
            slot16[r:r + 1, :] = slot_ref[0:1, r * 128:(r + 1) * 128]
        slot_t = slot16[...].T
        for r in range(16):
            slot_col[r] = jnp.broadcast_to(slot_t[:, r:r + 1], (128, 128))
        for i, piece in enumerate(thirds(particle_rows(pos_ref[...]))):
            rows_p[i * 32:(i + 1) * 32, :] = piece

    lane = lax.broadcasted_iota(jnp.int32, (128, 128), 1)

    def tile_step(t, _):
        base = lane + t * 128
        acc = jnp.zeros((96, 128), F32)
        for r in range(0, 16, 2):
            hot = jnp.concatenate([(slot_col[r + h] == base).astype(F32).astype(BF16) for h in (0, 1)], axis=0)
            acc = acc + jnp.dot(rows_p[:, r * 128:(r + 2) * 128], hot, preferred_element_type=F32)
        got = acc.astype(BF16)
        for g, piece in enumerate((0, 0, 0, 1, 1, 2)):
            feats[t, g * 16:(g + 1) * 16, 0:128] = got[piece * 32:piece * 32 + 16]
            feats[t, g * 16:(g + 1) * 16, 128:256] = got[piece * 32 + 16:piece * 32 + 32]
        where_p[t] = (-0.5 / RATE) * (acc[0:8] + acc[32:40] + acc[64:72])
        return 0

    def particle_tiles(n):
        lax.fori_loop(tiles_done[0], tiles_done[0] + n, tile_step, 0)
        tiles_done[0] += n

    def partner(g):
        for s in (0, 1):
            for k, qrel in enumerate((0, 3, 1, 2)):
                qp = lax.rem(qs[1 - s] + qrel, 4)
                arrived(refs[s].at[1 - c, qp, span(g)], cin_sem.at[s, g, k])

    def features(core, g):
        lo, hi = GROUPS[g]

        def step(j, _):
            at = lo + j
            for q in range(4):
                for p in (0, 2):
                    vals = []
                    for k in range(10):
                        if k < 6:
                            a, b = v3[core, q, at, p, 4 * k:4 * k + 4, :], v3[core, q, at, p + 1, 4 * k:4 * k + 4, :]
                        else:
                            r = 4 * k - 24
                            a, b = v2[core, p, at, q, r:r + 4, :], v2[core, p + 1, at, q, r:r + 4, :]
                        vals.append(jnp.concatenate([a, b], axis=0))
                    base = pl.multiple_of(((core * 4 + q) * 8 + at) * 256 + p * 64, 128)
                    for f, row in enumerate(node_rows(vals)):
                        nodes[pl.ds(base + f, 8, stride=16), :] = row
            return 0
        lax.fori_loop(0, hi - lo, step, 0)

    particle_prep()
    column(0)
    particle_tiles(2)
    column(1)
    particle_tiles(2)
    column(2)
    particle_tiles(2)
    ready(0)
    particle_tiles(3)
    ready(1)
    particle_tiles(3)
    ready(2)
    particle_tiles(4)
    side(0)
    side(1)
    side(2)
    far(0)
    features(c, 0)
    far(1)
    far(2)
    features(c, 1)
    partner(0)
    features(1 - c, 0)
    partner(1)
    features(1 - c, 1)
    features(c, 2)
    partner(2)
    features(1 - c, 2)
    for cp in sends:
        cp.wait_send()

def gather_nodes(nodes, pos, slots, counts, lists):
    dma = pltpu.SemaphoreType.DMA
    n = len(GROUPS)
    vmem = pl.BlockSpec(memory_space=pltpu.VMEM)
    hbm = pl.BlockSpec(memory_space=pltpu.HBM)
    return pl.pallas_call(
        gather_kernel,
        out_shape=[jax.ShapeDtypeStruct((1024 * 16, 128), F32),
                   jax.ShapeDtypeStruct((TILES, 96, 256), BF16),
                   jax.ShapeDtypeStruct((TILES, 8, 128), F32),
                   jax.ShapeDtypeStruct((16, 128), jnp.int32),
                   jax.ShapeDtypeStruct(counts.shape, jnp.int32),
                   jax.ShapeDtypeStruct(lists.shape, jnp.int32)],
        in_specs=[hbm] * 5,
        out_specs=[vmem] * 6,
        scratch_shapes=[pltpu.VMEM((2, NR, NZ, NR, 24, 128), F32), pltpu.VMEM((2, NR, NZ, NR, 16, 128), F32),
                        pltpu.VMEM((40, 128), F32), pltpu.VMEM((3, 2048), F32), pltpu.VMEM((1, 2048), jnp.int32),
                        pltpu.VMEM((96, 2048), BF16), pltpu.VMEM((16, 128, 128), jnp.int32),
                        pltpu.VMEM((8, 40, 128), F32), dma((5,)),
                        dma((2, n, 3)), dma((8,)), dma((2, n, 4)), dma((2, n, 4)),
                        dma((2, n, 3)), dma((8,)), dma((2, n, 4)), dma((2, n, 4)), dma((2, n))],
        compiler_params=pltpu.CompilerParams(collective_id=0, has_side_effects=True, vmem_limit_bytes=20 << 20),
        name="gather_nodes",
    )(*(pltpu.with_memory_space_constraint(a, pltpu.HBM) for a in (nodes, pos, slots, counts, lists)))


WIDE = 3
def halves(v):
    a = v.astype(BF16)
    return a, (v - a.astype(F32)).astype(BF16)

def force_kernel(counts_vmem, lists_vmem, nodes, feats, where_p, slot16, out_ref, left, sb, cols, high, low, total, forces, counts, lists, sems):
    fetch = [pltpu.make_async_copy(counts_vmem, counts, sems.at[0]), pltpu.make_async_copy(lists_vmem, lists, sems.at[1])]
    for cp in fetch:
        cp.start()
    own_z = (lax.axis_index("gy") >> 1) & 7
    for cp in fetch:
        cp.wait()
    total[...] = jnp.zeros_like(total)
    def block_row(b):
        d = b >> 2
        c, z = d & 1, ((d >> 1) - own_z) & 7
        z = jnp.where(z > 4, 16 - 2 * z, jnp.maximum(2 * z - 1, 0))
        x, y = ((d >> 3) & 2) | ((d >> 7) & 1), (d >> 5) & 3
        p = jnp.where(c == 0, x, y)
        q = jnp.where(c == 0, y, x)
        return ((((c * 4 + q) * 8 + z) * 4 + p) * 4 + (b & 3)) * 16

    live = lax.fori_loop(0, TILES, lambda t, n: n + counts[t], 0)

    def take(t, k):
        ok = t < TILES
        at = jnp.minimum(t, TILES - 1)
        row = block_row(jnp.where(ok, lists[at, k], 0))
        last = k + 1 >= counts[at]
        return (row, t), (jnp.where(ok & last, t + 1, t), jnp.where(last, 0, k + 1))

    def node_at(row):
        return nodes[pl.ds(pl.multiple_of(row, 16), 16), :]

    def sums(h, pair):
        hi, lo = halves(node_at(pair[0]))
        both = jnp.concatenate([hi, lo], axis=0)
        return (jnp.dot(both, high[h], preferred_element_type=F32)
                + jnp.dot(both.astype(F32), low[h], preferred_element_type=F32))

    def radial(h):
        for r in range(0, 128, 16):
            dist = sb[h, r:r + 16, 0:128]
            mass = jnp.broadcast_to(cols[h, r:r + 16, 15:16], (16, 128))
            trace = jnp.broadcast_to(cols[h, r:r + 16, 11:12], (16, 128))
            w = lax.rsqrt(dist)
            u = w * w
            v = pl.reciprocal(jnp.exp2(dist)) * u
            top = w + TOP[3]
            for coef in TOP[2::-1]:
                top = top * w + coef
            bottom = w + BOTTOM[2]
            for coef in BOTTOM[1::-1]:
                bottom = bottom * w + coef
            f0 = top * pl.reciprocal(bottom)
            f1 = f0 * u + FIRST
            f2 = f1 * u + SECOND
            both = (v * (mass * f0 + trace * f1 + sb[h, r:r + 16, 128:256] * f2), v * f1)
            for k, val in enumerate(both):
                hi = val.astype(BF16)
                high[h, r:r + 16, k * 128:k * 128 + 128] = hi
                low[h, r:r + 16, k * 128:k * 128 + 128] = val - hi.astype(F32)

    def products(h, pair):
        row, t = pair
        node = node_at(row)
        p1, p2, p3 = thirds(node)
        left[h] = jnp.concatenate([p1, p2, p3, p1, p2, p1], axis=0).T
        sb[h] = jnp.dot(left[h], feats[jnp.minimum(t, TILES - 1)], preferred_element_type=F32)
        cols[h, :, 0:16] = node.T

    idle = ((0, TILES),) * WIDE

    def pair_step(i, carry):
        at, first, second, third = carry
        got = [sums(h, third[h]) for h in range(WIDE)]
        for h in range(WIDE):
            radial(h)
        for h in range(WIDE):
            products(h, first[h])
        for h in range(WIDE):
            total[third[h][1]] += got[h]
        fresh = []
        for h in range(WIDE):
            pair, at = take(*at)
            fresh.append(pair)
        return at, tuple(fresh), first, second
    at = (0, 0)
    begin = []
    for h in range(WIDE):
        pair, at = take(*at)
        begin.append(pair)
    lax.fori_loop(0, (live + WIDE - 1) // WIDE + 2, pair_step, (at, tuple(begin), idle, idle))

    for t in range(TILES):
        s = total[t, 0:16, :] + total[t, 16:32, :]
        x, y, z = where_p[t, 0:1, :], where_p[t, 1:2, :], where_p[t, 2:3, :]
        rad = lambda k: s[k:k + 1, 0:128]
        sec = lambda k: s[k:k + 1, 128:256] * (SCALE * RATE**2)
        m = rad(4)
        xx, yy, xy, xz, yz = sec(9), sec(10), sec(12), sec(13), sec(14)
        zz = 2.0 * s[11:12, 128:256] - xx - yy
        forces[0, t:t + 1, :] = x * m - rad(0) + xx * x + xy * y + xz * z - sec(5)
        forces[1, t:t + 1, :] = y * m - rad(1) + xy * x + yy * y + yz * z - sec(6)
        forces[2, t:t + 1, :] = z * m - rad(2) + xz * x + yz * y + zz * z - sec(7)
    slot = slot16[...]
    at = slot % 128
    tile = slot // 128
    for k in range(3):
        got = jnp.zeros((16, 128), F32)
        for t in range(TILES):
            row = jnp.broadcast_to(forces[k, t:t + 1, :], (16, 128))
            got = jnp.where(tile == t, jnp.take_along_axis(row, at, axis=1), got)
        for r in range(16):
            out_ref[k:k + 1, r * 128:(r + 1) * 128] = got[r:r + 1, :]

def forces_of(counts, lists, nodes, feats, where_p, slots):
    vmem = pl.BlockSpec(memory_space=pltpu.VMEM)
    return pl.pallas_call(
        force_kernel,
        out_shape=jax.ShapeDtypeStruct((3, TILES * TILE), F32),
        in_specs=[vmem] * 6,
        out_specs=vmem,
        scratch_shapes=[pltpu.VMEM((WIDE, 128, 96), BF16), pltpu.VMEM((WIDE, 128, 256), F32), pltpu.VMEM((WIDE, 128, 128), F32),
                        pltpu.VMEM((WIDE, 128, 256), BF16), pltpu.VMEM((WIDE, 128, 256), F32), pltpu.VMEM((17, 32, 256), F32), pltpu.VMEM((3, 16, 128), F32),
                        pltpu.SMEM((16,), jnp.int32), pltpu.SMEM((16, 16), jnp.int32), pltpu.SemaphoreType.DMA((2,))],
        compiler_params=pltpu.CompilerParams(vmem_limit_bytes=16 << 20),
        name="tile_forces",
    )(counts, lists, nodes, feats, where_p, slots)


def shards(positions, node_moments, slot_of, block_list, tile_counts):
    nodes, feats, where_p, slots, counts, lists = gather_nodes(
        node_moments, positions, slot_of, tile_counts, block_list
    )
    return forces_of(counts, lists, nodes, feats, where_p, slots)


def solution(mesh):
    placed = (
        P(None, ("gx", "gy")),
        P(None, ("gx", "gy")),
        P(("gx", "gy"), None),
        P(("gx", "gy"), None),
        P(("gx", "gy")),
    )
    return jax.shard_map(
        shards, mesh=mesh, in_specs=placed, out_specs=P(None, ("gx", "gy")), check_vma=False
    )
```

```python
import functools
import math

import jax
import jax.numpy as jnp
from jax import lax
from jax.experimental import pallas as pl
from jax.experimental.pallas import tpu as pltpu
from jax.sharding import PartitionSpec as P

F32 = jnp.float32
BF16 = jnp.bfloat16
TILE = 128
TILES = 16
RATE = 0.25 * math.log2(math.e)
SCALE = 3.00002466 * math.sqrt(RATE)
TOP = (0.137173002, 0.67870502, 1.41669777, 1.3963634)
BOTTOM = (0.145984292, 0.723140227, 1.39646547)
ROOT_PI = math.sqrt(math.pi)
FIRST = 0.5 / ROOT_PI / (SCALE * RATE)
SECOND = 0.05 / ROOT_PI / (SCALE * RATE**2)
MESH = pl.DeviceIdType.MESH
NZ = 8
NR = 4

def thirds(v):
    a = v.astype(BF16)
    r = v - a.astype(F32)
    b = r.astype(BF16)
    return a, b, (r - b.astype(F32)).astype(BF16)

def particle_rows(pos):
    x = pos[0:1] - 2.0
    y = pos[1:2] - 2.0
    z = pos[2:3] - 2.0
    none = jnp.zeros_like(x)
    xx, yy, zz = x * x, y * y, z * z
    g = -2.5 * SCALE * RATE**3
    dist = [-2.0 * RATE * x, -2.0 * RATE * y, -2.0 * RATE * z, none + RATE, RATE * (xx + yy + zz)] + [none] * 11
    quad = [none] * 5 + [-2.0 * g * x, -2.0 * g * y, -2.0 * g * z, none + g, g * (xx - zz), g * (yy - zz), -5.0 * RATE * zz,
            2.0 * g * (x * y), 2.0 * g * (x * z), 2.0 * g * (y * z), none]
    return jnp.concatenate(dist + quad, axis=0)

def node_rows(v):
    mass = v[0]
    x, y, z = v[1] - 2.0, v[2] - 2.0, v[3] - 2.0
    qxx, qyy, qzz, qxy, qxz, qyz = v[4:]
    qcx = qxx * x + qxy * y + qxz * z
    qcy = qxy * x + qyy * y + qyz * z
    qcz = qxz * x + qyz * y + qzz * z
    return [x, y, z, x * x + y * y + z * z + 0.25, jnp.ones_like(x), qcx, qcy, qcz,
            x * qcx + y * qcy + z * qcz, qxx, qyy, (0.5 * SCALE * RATE**2) * (qxx + qyy + qzz), qxy, qxz, qyz,
            (-SCALE * RATE / 3.0) * mass]

def device_of(first, p, q, z, c):
    x = first * p + (1 - first) * q
    y = first * q + (1 - first) * p
    return (lax.rem(x, 2) * 4 + y, (x // 2) * 16 + z * 2 + c)

ZPOS = (0, 1, 3, 5, 7, 6, 4, 2)
GROUPS = ((0, 1), (1, 3), (3, 6), (6, 8))
P_STEPS = ((0, 1), (1, 3), (2, 2))
Z_STEPS = (1, 7, 2, 6, 3, 5, 4)

def gather_kernel(nodes_hbm, pos_hbm, slot_hbm, counts_hbm, lists_hbm, nodes, feats, where_p, slot16, counts, lists,
                  v3, v2, own_ref, pos_ref, slot_ref, rows_p, slot_col, stage, load_sem, pin_sem, zin_sem, qin_sem, cin_sem, psend, zsend, qsend, csend, own_sem):
    gx = lax.axis_index("gx")
    gy = lax.axis_index("gy")
    c = lax.rem(gy, 2)
    z = lax.rem(gy // 2, 8)
    x = (gy // 16) * 2 + gx // 4
    y = lax.rem(gx, 4)
    refs = (v3, v2)
    rows = ((0, 24), (24, 16))
    firsts = (1 - c, c)
    ps = tuple(f * x + (1 - f) * y for f in firsts)
    qs = tuple(f * y + (1 - f) * x for f in firsts)

    def dev(s, p, q, zz, cc):
        return device_of(firsts[s], lax.rem(p, 4), lax.rem(q, 4), lax.rem(zz, 8), cc)

    def qat(s, rel):
        return lax.rem(qs[s] + rel, 4)

    def span(g):
        lo, hi = GROUPS[g]
        return pl.ds(lo, hi - lo)

    for q in range(10):
        for b in range(4):
            pltpu.make_async_copy(nodes_hbm.at[pl.ds(q, 1), pl.ds(b * 128, 128)], own_ref.at[pl.ds(q * 4 + b, 1)], load_sem.at[0]).start()
    fetch = [pltpu.make_async_copy(pos_hbm, pos_ref, load_sem.at[1]), pltpu.make_async_copy(slot_hbm, slot_ref, load_sem.at[2]),
             pltpu.make_async_copy(counts_hbm, counts, load_sem.at[3]), pltpu.make_async_copy(lists_hbm, lists, load_sem.at[4])]
    for cp in fetch:
        cp.start()

    barrier = pltpu.get_barrier_semaphore()
    peers = [device_of(1, x, y, z, 1 - c)]
    for d in (1, 2, 3):
        peers.append(device_of(1, lax.rem(x + d, 4), y, z, c))
        peers.append(device_of(1, x, lax.rem(y + d, 4), z, c))
    for d in range(1, 8):
        peers.append(device_of(1, x, y, lax.rem(z + d, 8), c))
    for peer in peers:
        pl.semaphore_signal(barrier, inc=1, device_id=peer, device_id_type=MESH)
    pltpu.make_async_copy(own_ref, own_ref, load_sem.at[0]).wait()
    pl.semaphore_wait(barrier, len(peers))

    sends = []

    def send(src, dst, ssem, rsem, to):
        cp = pltpu.make_async_remote_copy(src_ref=src, dst_ref=dst, send_sem=ssem, recv_sem=rsem, device_id=to, device_id_type=MESH)
        cp.start()
        sends.append(cp)

    def arrived(ref, sem):
        pltpu.make_async_remote_copy(src_ref=ref, dst_ref=ref, send_sem=sem, recv_sem=sem, device_id=(gx, gy), device_id_type=MESH).wait_recv()

    for d in Z_STEPS:
        pos = ZPOS[8 - d]
        send(own_ref, stage.at[pos], zsend.at[pos], zin_sem.at[pos], dev(0, ps[0], qs[0], z + d, c))
    local = {}

    def column(g):
        lo, hi = GROUPS[g]
        for pos in range(max(lo, 1), hi):
            arrived(stage.at[pos], zin_sem.at[pos])
        for s in (0, 1):
            r0, rn = rows[s]
            src = own_ref.at[pl.ds(r0, rn)] if hi == 1 else stage.at[span(g), pl.ds(r0, rn)]
            at = 0 if hi == 1 else span(g)
            dst = refs[s].at[c, qs[s], at, ps[s]]
            for i, d in P_STEPS:
                send(src, dst, psend.at[s, g, i], pin_sem.at[s, g, i], dev(s, ps[s] + d, qs[s], z, c))
            cp = pltpu.make_async_copy(src, dst, own_sem.at[s, g])
            cp.start()
            local[s, g] = cp

    def bundle(s, qrel, g):
        return refs[s].at[c, qat(s, qrel), span(g)]

    def ready(g):
        lo, hi = GROUPS[g]
        for s in (0, 1):
            for i, d in P_STEPS:
                at = 0 if hi == 1 else span(g)
                arrived(refs[s].at[c, qs[s], at, lax.rem(ps[s] + 4 - d, 4)], pin_sem.at[s, g, i])
            local[s, g].wait()
            b = bundle(s, 0, g)
            send(b, b, qsend.at[s, g, 0], qin_sem.at[s, g, 0], dev(s, ps[s], qs[s] + 1, z, c))
            send(b, b, qsend.at[s, g, 1], qin_sem.at[s, g, 1], dev(s, ps[s], qs[s] + 3, z, c))
            send(b, b, csend.at[s, g, 0], cin_sem.at[s, g, 0], dev(s, ps[s], qs[s], z, 1 - c))

    def side(g):
        for s in (0, 1):
            for i, rel in ((0, 3), (1, 1)):
                b = bundle(s, rel, g)
                arrived(b, qin_sem.at[s, g, i])
                h = refs[s].at[c, qat(s, rel), span(g), pl.ds(2 * i, 2)]
                send(h, h, qsend.at[s, g, 2 + i], qin_sem.at[s, g, 2 + i], dev(s, ps[s], qs[s] + (1 if i == 0 else 3), z, c))
                send(b, b, csend.at[s, g, 1 + i], cin_sem.at[s, g, 1 + i], dev(s, ps[s], qs[s], z, 1 - c))

    def far(g):
        for s in (0, 1):
            for i in (0, 1):
                arrived(refs[s].at[c, qat(s, 2), span(g), pl.ds(2 * i, 2)], qin_sem.at[s, g, 2 + i])
            b = bundle(s, 2, g)
            send(b, b, csend.at[s, g, 3], cin_sem.at[s, g, 3], dev(s, ps[s], qs[s], z, 1 - c))

    tiles_done = [0]

    def particle_prep():
        for cp in fetch:
            cp.wait()
        for r in range(16):
            slot16[r:r + 1, :] = slot_ref[0:1, r * 128:(r + 1) * 128]
        slot_t = slot16[...].T
        for r in range(16):
            slot_col[r] = jnp.broadcast_to(slot_t[:, r:r + 1], (128, 128))
        for i, piece in enumerate(thirds(particle_rows(pos_ref[...]))):
            rows_p[i * 32:(i + 1) * 32, :] = piece

    lane = lax.broadcasted_iota(jnp.int32, (128, 128), 1)

    def tile_step(t, _):
        base = lane + t * 128
        acc = jnp.zeros((96, 128), F32)
        for r in range(0, 16, 2):
            hot = jnp.concatenate([(slot_col[r + h] == base).astype(F32).astype(BF16) for h in (0, 1)], axis=0)
            acc = acc + jnp.dot(rows_p[:, r * 128:(r + 2) * 128], hot, preferred_element_type=F32)
        got = acc.astype(BF16)
        for g, piece in enumerate((0, 0, 0, 1, 1, 2)):
            feats[t, g * 16:(g + 1) * 16, 0:128] = got[piece * 32:piece * 32 + 16]
            feats[t, g * 16:(g + 1) * 16, 128:256] = got[piece * 32 + 16:piece * 32 + 32]
        where_p[t] = (-0.5 / RATE) * (acc[0:8] + acc[32:40] + acc[64:72])
        return 0

    def particle_tiles(n):
        lax.fori_loop(tiles_done[0], tiles_done[0] + n, tile_step, 0)
        tiles_done[0] += n

    def partner(g):
        for s in (0, 1):
            for k, qrel in enumerate((0, 3, 1, 2)):
                qp = lax.rem(qs[1 - s] + qrel, 4)
                arrived(refs[s].at[1 - c, qp, span(g)], cin_sem.at[s, g, k])

    def features(core, g):
        lo, hi = GROUPS[g]

        def step(j, _):
            at = lo + j
            for q in range(4):
                for p in (0, 2):
                    vals = []
                    for k in range(10):
                        if k < 6:
                            a, b = v3[core, q, at, p, 4 * k:4 * k + 4, :], v3[core, q, at, p + 1, 4 * k:4 * k + 4, :]
                        else:
                            r = 4 * k - 24
                            a, b = v2[core, p, at, q, r:r + 4, :], v2[core, p + 1, at, q, r:r + 4, :]
                        vals.append(jnp.concatenate([a, b], axis=0))
                    base = pl.multiple_of(((core * 4 + q) * 8 + at) * 256 + p * 64, 128)
                    for f, row in enumerate(node_rows(vals)):
                        nodes[pl.ds(base + f, 8, stride=16), :] = row
            return 0
        lax.fori_loop(0, hi - lo, step, 0)

    column(0)
    particle_prep()
    particle_tiles(8)
    column(1)
    particle_tiles(2)
    column(2)
    column(3)
    ready(0)
    ready(1)
    particle_tiles(2)
    ready(2)
    particle_tiles(2)
    ready(3)
    particle_tiles(2)
    side(0)
    side(1)
    side(2)
    side(3)
    far(0)
    features(c, 0)
    far(1)
    features(c, 1)
    far(2)
    far(3)
    features(c, 2)
    partner(0)
    features(1 - c, 0)
    partner(1)
    features(1 - c, 1)
    partner(2)
    features(1 - c, 2)
    features(c, 3)
    partner(3)
    features(1 - c, 3)
    for cp in sends:
        cp.wait_send()

def gather_nodes(nodes, pos, slots, counts, lists):
    dma = pltpu.SemaphoreType.DMA
    n = len(GROUPS)
    vmem = pl.BlockSpec(memory_space=pltpu.VMEM)
    hbm = pl.BlockSpec(memory_space=pltpu.HBM)
    return pl.pallas_call(
        gather_kernel,
        out_shape=[jax.ShapeDtypeStruct((1024 * 16, 128), F32),
                   jax.ShapeDtypeStruct((TILES, 96, 256), BF16),
                   jax.ShapeDtypeStruct((TILES, 8, 128), F32),
                   jax.ShapeDtypeStruct((16, 128), jnp.int32),
                   jax.ShapeDtypeStruct(counts.shape, jnp.int32),
                   jax.ShapeDtypeStruct(lists.shape, jnp.int32)],
        in_specs=[hbm] * 5,
        out_specs=[vmem] * 6,
        scratch_shapes=[pltpu.VMEM((2, NR, NZ, NR, 24, 128), F32), pltpu.VMEM((2, NR, NZ, NR, 16, 128), F32),
                        pltpu.VMEM((40, 128), F32), pltpu.VMEM((3, 2048), F32), pltpu.VMEM((1, 2048), jnp.int32),
                        pltpu.VMEM((96, 2048), BF16), pltpu.VMEM((16, 128, 128), jnp.int32),
                        pltpu.VMEM((8, 40, 128), F32), dma((5,)),
                        dma((2, n, 3)), dma((8,)), dma((2, n, 4)), dma((2, n, 4)),
                        dma((2, n, 3)), dma((8,)), dma((2, n, 4)), dma((2, n, 4)), dma((2, n))],
        compiler_params=pltpu.CompilerParams(collective_id=0, has_side_effects=True, vmem_limit_bytes=20 << 20),
        name="gather_nodes",
    )(*(pltpu.with_memory_space_constraint(a, pltpu.HBM) for a in (nodes, pos, slots, counts, lists)))


WIDE = 3
def halves(v):
    a = v.astype(BF16)
    return a, (v - a.astype(F32)).astype(BF16)

def force_kernel(counts_vmem, lists_vmem, nodes, feats, where_p, slot16, out_ref, sb, cols, high, low, total, forces, counts, lists, sems):
    fetch = [pltpu.make_async_copy(counts_vmem, counts, sems.at[0]), pltpu.make_async_copy(lists_vmem, lists, sems.at[1])]
    for cp in fetch:
        cp.start()
    own_z = (lax.axis_index("gy") >> 1) & 7
    for cp in fetch:
        cp.wait()
    total[...] = jnp.zeros_like(total)
    def block_row(b):
        d = b >> 2
        c, z = d & 1, ((d >> 1) - own_z) & 7
        z = jnp.where(z > 4, 16 - 2 * z, jnp.maximum(2 * z - 1, 0))
        x, y = ((d >> 3) & 2) | ((d >> 7) & 1), (d >> 5) & 3
        p = jnp.where(c == 0, x, y)
        q = jnp.where(c == 0, y, x)
        return ((((c * 4 + q) * 8 + z) * 4 + p) * 4 + (b & 3)) * 16

    live = lax.fori_loop(0, TILES, lambda t, n: n + counts[t], 0)

    def take(t, k):
        ok = t < TILES
        at = jnp.minimum(t, TILES - 1)
        row = block_row(jnp.where(ok, lists[at, k], 0))
        last = k + 1 >= counts[at]
        return (row, t), (jnp.where(ok & last, t + 1, t), jnp.where(last, 0, k + 1))

    def node_at(row):
        return nodes[pl.ds(pl.multiple_of(row, 16), 16), :]

    def sums(h, pair):
        hi, lo = halves(node_at(pair[0]))
        both = jnp.concatenate([hi, lo], axis=0)
        return (jnp.dot(both, high[h], preferred_element_type=F32)
                + jnp.dot(both.astype(F32), low[h], preferred_element_type=F32))

    def radial(h):
        for r in range(0, 128, 8):
            dist = sb[h, r:r + 8, 0:128]
            mass = jnp.broadcast_to(cols[h, r:r + 8, 15:16], (8, 128))
            trace = jnp.broadcast_to(cols[h, r:r + 8, 11:12], (8, 128))
            w = lax.rsqrt(dist)
            u = w * w
            v = jnp.exp2(-dist) * u
            top = w + TOP[3]
            for coef in TOP[2::-1]:
                top = top * w + coef
            bottom = w + BOTTOM[2]
            for coef in BOTTOM[1::-1]:
                bottom = bottom * w + coef
            f0 = top * pl.reciprocal(bottom)
            f1 = f0 * u + FIRST
            f2 = f1 * u + SECOND
            both = (v * (mass * f0 + trace * f1 + sb[h, r:r + 8, 128:256] * f2), v * f1)
            for k, val in enumerate(both):
                hi = val.astype(BF16)
                high[h, r:r + 8, k * 128:k * 128 + 128] = hi
                low[h, r:r + 8, k * 128:k * 128 + 128] = val - hi.astype(F32)

    def products(h, pair):
        row, t = pair
        node = node_at(row)
        p1, p2, p3 = thirds(node)
        sb[h] = jnp.dot(jnp.concatenate([p1, p2, p3, p1, p2, p1], axis=0).T, feats[jnp.minimum(t, TILES - 1)], preferred_element_type=F32)
        cols[h, :, 0:16] = node.T

    idle = ((0, TILES),) * WIDE

    def pair_step(i, carry):
        at, first, second, third = carry
        got = [sums(h, third[h]) for h in range(WIDE)]
        for h in range(WIDE):
            radial(h)
        for h in range(WIDE):
            products(h, first[h])
        for h in range(WIDE):
            total[third[h][1]] += got[h]
        fresh = []
        for h in range(WIDE):
            pair, at = take(*at)
            fresh.append(pair)
        return at, tuple(fresh), first, second
    at = (0, 0)
    begin = []
    for h in range(WIDE):
        pair, at = take(*at)
        begin.append(pair)
    lax.fori_loop(0, (live + WIDE - 1) // WIDE + 2, pair_step, (at, tuple(begin), idle, idle))

    for t in range(TILES):
        s = total[t, 0:16, :] + total[t, 16:32, :]
        x, y, z = where_p[t, 0:1, :], where_p[t, 1:2, :], where_p[t, 2:3, :]
        rad = lambda k: s[k:k + 1, 0:128]
        sec = lambda k: s[k:k + 1, 128:256] * (SCALE * RATE**2)
        m = rad(4)
        xx, yy, xy, xz, yz = sec(9), sec(10), sec(12), sec(13), sec(14)
        zz = 2.0 * s[11:12, 128:256] - xx - yy
        forces[0, t:t + 1, :] = x * m - rad(0) + xx * x + xy * y + xz * z - sec(5)
        forces[1, t:t + 1, :] = y * m - rad(1) + xy * x + yy * y + yz * z - sec(6)
        forces[2, t:t + 1, :] = z * m - rad(2) + xz * x + yz * y + zz * z - sec(7)
    slot = slot16[...]
    at = slot % 128
    tile = slot // 128
    for k in range(3):
        got = jnp.zeros((16, 128), F32)
        for t in range(TILES):
            row = jnp.broadcast_to(forces[k, t:t + 1, :], (16, 128))
            got = jnp.where(tile == t, jnp.take_along_axis(row, at, axis=1), got)
        for r in range(16):
            out_ref[k:k + 1, r * 128:(r + 1) * 128] = got[r:r + 1, :]

def forces_of(counts, lists, nodes, feats, where_p, slots):
    vmem = pl.BlockSpec(memory_space=pltpu.VMEM)
    return pl.pallas_call(
        force_kernel,
        out_shape=jax.ShapeDtypeStruct((3, TILES * TILE), F32),
        in_specs=[vmem] * 6,
        out_specs=vmem,
        scratch_shapes=[pltpu.VMEM((WIDE, 128, 256), F32), pltpu.VMEM((WIDE, 128, 128), F32),
                        pltpu.VMEM((WIDE, 128, 256), BF16), pltpu.VMEM((WIDE, 128, 256), F32), pltpu.VMEM((17, 32, 256), F32), pltpu.VMEM((3, 16, 128), F32),
                        pltpu.SMEM((16,), jnp.int32), pltpu.SMEM((16, 16), jnp.int32), pltpu.SemaphoreType.DMA((2,))],
        compiler_params=pltpu.CompilerParams(vmem_limit_bytes=16 << 20),
        name="tile_forces",
    )(counts, lists, nodes, feats, where_p, slots)


def shards(positions, node_moments, slot_of, block_list, tile_counts):
    nodes, feats, where_p, slots, counts, lists = gather_nodes(
        node_moments, positions, slot_of, tile_counts, block_list
    )
    return forces_of(counts, lists, nodes, feats, where_p, slots)


def solution(mesh):
    placed = (
        P(None, ("gx", "gy")),
        P(None, ("gx", "gy")),
        P(("gx", "gy"), None),
        P(("gx", "gy"), None),
        P(("gx", "gy")),
    )
    return jax.shard_map(
        shards, mesh=mesh, in_specs=placed, out_specs=P(None, ("gx", "gy")), check_vma=False
    )
```

```python
import functools
import math

import jax
import jax.numpy as jnp
from jax import lax
from jax.experimental import pallas as pl
from jax.experimental.pallas import tpu as pltpu
from jax.sharding import PartitionSpec as P

F32 = jnp.float32
BF16 = jnp.bfloat16
TILE = 128
TILES = 16
RATE = 0.25 * math.log2(math.e)
SCALE = 3.00002466 * math.sqrt(RATE)
TOP = (0.137173002, 0.67870502, 1.41669777, 1.3963634)
BOTTOM = (0.145984292, 0.723140227, 1.39646547)
ROOT_PI = math.sqrt(math.pi)
FIRST = 0.5 / ROOT_PI / (SCALE * RATE)
SECOND = 0.05 / ROOT_PI / (SCALE * RATE**2)
MESH = pl.DeviceIdType.MESH
NZ = 8
NR = 4

def thirds(v):
    a = v.astype(BF16)
    r = v - a.astype(F32)
    b = r.astype(BF16)
    return a, b, (r - b.astype(F32)).astype(BF16)

def particle_rows(pos):
    x = pos[0:1] - 2.0
    y = pos[1:2] - 2.0
    z = pos[2:3] - 2.0
    none = jnp.zeros_like(x)
    xx, yy, zz = x * x, y * y, z * z
    g = -2.5 * SCALE * RATE**3
    dist = [-2.0 * RATE * x, -2.0 * RATE * y, -2.0 * RATE * z, none + RATE, RATE * (xx + yy + zz)] + [none] * 11
    quad = [none] * 5 + [-2.0 * g * x, -2.0 * g * y, -2.0 * g * z, none + g, g * (xx - zz), g * (yy - zz), -5.0 * RATE * zz,
            2.0 * g * (x * y), 2.0 * g * (x * z), 2.0 * g * (y * z), none]
    return jnp.concatenate(dist + quad, axis=0)

def node_rows(v):
    mass = v[0]
    x, y, z = v[1] - 2.0, v[2] - 2.0, v[3] - 2.0
    qxx, qyy, qzz, qxy, qxz, qyz = v[4:]
    qcx = qxx * x + qxy * y + qxz * z
    qcy = qxy * x + qyy * y + qyz * z
    qcz = qxz * x + qyz * y + qzz * z
    return [x, y, z, x * x + y * y + z * z + 0.25, jnp.ones_like(x), qcx, qcy, qcz,
            x * qcx + y * qcy + z * qcz, qxx, qyy, (0.5 * SCALE * RATE**2) * (qxx + qyy + qzz), qxy, qxz, qyz,
            (-SCALE * RATE / 3.0) * mass]

def device_of(first, p, q, z, c):
    x = first * p + (1 - first) * q
    y = first * q + (1 - first) * p
    return (lax.rem(x, 2) * 4 + y, (x // 2) * 16 + z * 2 + c)

ZPOS = (0, 1, 3, 5, 7, 6, 4, 2)
GROUPS = ((0, 1), (1, 3), (3, 6), (6, 8))
P_STEPS = ((0, 1), (1, 3), (2, 2))
Z_STEPS = (1, 7, 2, 6, 3, 5, 4)

def gather_kernel(nodes_hbm, pos_hbm, slot_hbm, counts_hbm, lists_hbm, nodes, feats, where_p, slot16, counts, lists,
                  v3, v2, own_ref, pos_ref, slot_ref, rows_p, slot_col, stage, load_sem, pin_sem, zin_sem, qin_sem, cin_sem, psend, zsend, qsend, csend, own_sem):
    gx = lax.axis_index("gx")
    gy = lax.axis_index("gy")
    c = lax.rem(gy, 2)
    z = lax.rem(gy // 2, 8)
    x = (gy // 16) * 2 + gx // 4
    y = lax.rem(gx, 4)
    refs = (v3, v2)
    rows = ((0, 24), (24, 16))
    firsts = (1 - c, c)
    ps = tuple(f * x + (1 - f) * y for f in firsts)
    qs = tuple(f * y + (1 - f) * x for f in firsts)

    def dev(s, p, q, zz, cc):
        return device_of(firsts[s], lax.rem(p, 4), lax.rem(q, 4), lax.rem(zz, 8), cc)

    def qat(s, rel):
        return lax.rem(qs[s] + rel, 4)

    def span(g):
        lo, hi = GROUPS[g]
        return pl.ds(lo, hi - lo)

    for q in range(10):
        for b in range(4):
            pltpu.make_async_copy(nodes_hbm.at[pl.ds(q, 1), pl.ds(b * 128, 128)], own_ref.at[pl.ds(q * 4 + b, 1)], load_sem.at[0]).start()
    fetch = [pltpu.make_async_copy(pos_hbm, pos_ref, load_sem.at[1]), pltpu.make_async_copy(slot_hbm, slot_ref, load_sem.at[2]),
             pltpu.make_async_copy(counts_hbm, counts, load_sem.at[3]), pltpu.make_async_copy(lists_hbm, lists, load_sem.at[4])]
    for cp in fetch:
        cp.start()

    barrier = pltpu.get_barrier_semaphore()
    peers = [device_of(1, x, y, z, 1 - c)]
    for d in (1, 2, 3):
        peers.append(device_of(1, lax.rem(x + d, 4), y, z, c))
        peers.append(device_of(1, x, lax.rem(y + d, 4), z, c))
    for d in range(1, 8):
        peers.append(device_of(1, x, y, lax.rem(z + d, 8), c))
    for peer in peers:
        pl.semaphore_signal(barrier, inc=1, device_id=peer, device_id_type=MESH)
    pltpu.make_async_copy(own_ref, own_ref, load_sem.at[0]).wait()
    pl.semaphore_wait(barrier, len(peers))

    sends = []

    def send(src, dst, ssem, rsem, to):
        cp = pltpu.make_async_remote_copy(src_ref=src, dst_ref=dst, send_sem=ssem, recv_sem=rsem, device_id=to, device_id_type=MESH)
        cp.start()
        sends.append(cp)

    def arrived(ref, sem):
        pltpu.make_async_remote_copy(src_ref=ref, dst_ref=ref, send_sem=sem, recv_sem=sem, device_id=(gx, gy), device_id_type=MESH).wait_recv()

    for d in Z_STEPS:
        pos = ZPOS[8 - d]
        send(own_ref, stage.at[pos], zsend.at[pos], zin_sem.at[pos], dev(0, ps[0], qs[0], z + d, c))
    local = {}

    def column(g):
        lo, hi = GROUPS[g]
        for pos in range(max(lo, 1), hi):
            arrived(stage.at[pos], zin_sem.at[pos])
        for s in (0, 1):
            r0, rn = rows[s]
            src = own_ref.at[pl.ds(r0, rn)] if hi == 1 else stage.at[span(g), pl.ds(r0, rn)]
            at = 0 if hi == 1 else span(g)
            dst = refs[s].at[c, qs[s], at, ps[s]]
            for i, d in P_STEPS:
                send(src, dst, psend.at[s, g, i], pin_sem.at[s, g, i], dev(s, ps[s] + d, qs[s], z, c))
            cp = pltpu.make_async_copy(src, dst, own_sem.at[s, g])
            cp.start()
            local[s, g] = cp

    def bundle(s, qrel, g):
        return refs[s].at[c, qat(s, qrel), span(g)]

    def ready(g):
        lo, hi = GROUPS[g]
        for s in (0, 1):
            for i, d in P_STEPS:
                at = 0 if hi == 1 else span(g)
                arrived(refs[s].at[c, qs[s], at, lax.rem(ps[s] + 4 - d, 4)], pin_sem.at[s, g, i])
            local[s, g].wait()
            b = bundle(s, 0, g)
            send(b, b, qsend.at[s, g, 0], qin_sem.at[s, g, 0], dev(s, ps[s], qs[s] + 1, z, c))
            send(b, b, qsend.at[s, g, 1], qin_sem.at[s, g, 1], dev(s, ps[s], qs[s] + 3, z, c))
            send(b, b, csend.at[s, g, 0], cin_sem.at[s, g, 0], dev(s, ps[s], qs[s], z, 1 - c))

    def side(g):
        for s in (0, 1):
            for i, rel in ((0, 3), (1, 1)):
                b = bundle(s, rel, g)
                arrived(b, qin_sem.at[s, g, i])
                h = refs[s].at[c, qat(s, rel), span(g), pl.ds(2 * i, 2)]
                send(h, h, qsend.at[s, g, 2 + i], qin_sem.at[s, g, 2 + i], dev(s, ps[s], qs[s] + (1 if i == 0 else 3), z, c))
                send(b, b, csend.at[s, g, 1 + i], cin_sem.at[s, g, 1 + i], dev(s, ps[s], qs[s], z, 1 - c))

    def far(g):
        for s in (0, 1):
            for i in (0, 1):
                h = refs[s].at[c, qat(s, 2), span(g), pl.ds(2 * i, 2)]
                arrived(h, qin_sem.at[s, g, 2 + i])
                send(h, h, csend.at[s, g, 3 + i], cin_sem.at[s, g, 3 + i], dev(s, ps[s], qs[s], z, 1 - c))

    tiles_done = [0]

    def particle_prep():
        for cp in fetch:
            cp.wait()
        for r in range(16):
            slot16[r:r + 1, :] = slot_ref[0:1, r * 128:(r + 1) * 128]
        slot_t = slot16[...].T
        for r in range(16):
            slot_col[r] = jnp.broadcast_to(slot_t[:, r:r + 1], (128, 128))
        for i, piece in enumerate(thirds(particle_rows(pos_ref[...]))):
            rows_p[i * 32:(i + 1) * 32, :] = piece

    lane = lax.broadcasted_iota(jnp.int32, (128, 128), 1)

    def tile_step(t, _):
        base = lane + t * 128
        acc = jnp.zeros((96, 128), F32)
        for r in range(0, 16, 2):
            hot = jnp.concatenate([(slot_col[r + h] == base).astype(F32).astype(BF16) for h in (0, 1)], axis=0)
            acc = acc + jnp.dot(rows_p[:, r * 128:(r + 2) * 128], hot, preferred_element_type=F32)
        got = acc.astype(BF16)
        for g, piece in enumerate((0, 0, 0, 1, 1, 2)):
            feats[t, g * 16:(g + 1) * 16, 0:128] = got[piece * 32:piece * 32 + 16]
            feats[t, g * 16:(g + 1) * 16, 128:256] = got[piece * 32 + 16:piece * 32 + 32]
        where_p[t] = (-0.5 / RATE) * (acc[0:8] + acc[32:40] + acc[64:72])
        return 0

    def particle_tiles(n):
        lax.fori_loop(tiles_done[0], tiles_done[0] + n, tile_step, 0)
        tiles_done[0] += n

    def partner(g):
        for s in (0, 1):
            for k, qrel in enumerate((0, 3, 1)):
                qp = lax.rem(qs[1 - s] + qrel, 4)
                arrived(refs[s].at[1 - c, qp, span(g)], cin_sem.at[s, g, k])
            for i in (0, 1):
                qp = lax.rem(qs[1 - s] + 2, 4)
                arrived(refs[s].at[1 - c, qp, span(g), pl.ds(2 * i, 2)], cin_sem.at[s, g, 3 + i])

    def features(core, g):
        lo, hi = GROUPS[g]

        def step(j, _):
            at = lo + j
            for q in range(4):
                for p in (0, 2):
                    vals = []
                    for k in range(10):
                        if k < 6:
                            a, b = v3[core, q, at, p, 4 * k:4 * k + 4, :], v3[core, q, at, p + 1, 4 * k:4 * k + 4, :]
                        else:
                            r = 4 * k - 24
                            a, b = v2[core, p, at, q, r:r + 4, :], v2[core, p + 1, at, q, r:r + 4, :]
                        vals.append(jnp.concatenate([a, b], axis=0))
                    base = pl.multiple_of(((core * 4 + q) * 8 + at) * 256 + p * 64, 128)
                    for f, row in enumerate(node_rows(vals)):
                        nodes[pl.ds(base + f, 8, stride=16), :] = row
            return 0
        lax.fori_loop(0, hi - lo, step, 0)

    column(0)
    particle_prep()
    particle_tiles(8)
    column(1)
    particle_tiles(2)
    column(2)
    column(3)
    ready(0)
    ready(1)
    particle_tiles(2)
    ready(2)
    particle_tiles(2)
    ready(3)
    particle_tiles(2)
    side(0)
    side(1)
    side(2)
    side(3)
    far(0)
    features(c, 0)
    far(1)
    features(c, 1)
    far(2)
    far(3)
    features(c, 2)
    partner(0)
    features(1 - c, 0)
    partner(1)
    features(1 - c, 1)
    partner(2)
    features(1 - c, 2)
    features(c, 3)
    partner(3)
    features(1 - c, 3)
    for cp in sends:
        cp.wait_send()

def gather_nodes(nodes, pos, slots, counts, lists):
    dma = pltpu.SemaphoreType.DMA
    n = len(GROUPS)
    vmem = pl.BlockSpec(memory_space=pltpu.VMEM)
    hbm = pl.BlockSpec(memory_space=pltpu.HBM)
    return pl.pallas_call(
        gather_kernel,
        out_shape=[jax.ShapeDtypeStruct((1024 * 16, 128), F32),
                   jax.ShapeDtypeStruct((TILES, 96, 256), BF16),
                   jax.ShapeDtypeStruct((TILES, 8, 128), F32),
                   jax.ShapeDtypeStruct((16, 128), jnp.int32),
                   jax.ShapeDtypeStruct(counts.shape, jnp.int32),
                   jax.ShapeDtypeStruct(lists.shape, jnp.int32)],
        in_specs=[hbm] * 5,
        out_specs=[vmem] * 6,
        scratch_shapes=[pltpu.VMEM((2, NR, NZ, NR, 24, 128), F32), pltpu.VMEM((2, NR, NZ, NR, 16, 128), F32),
                        pltpu.VMEM((40, 128), F32), pltpu.VMEM((3, 2048), F32), pltpu.VMEM((1, 2048), jnp.int32),
                        pltpu.VMEM((96, 2048), BF16), pltpu.VMEM((16, 128, 128), jnp.int32),
                        pltpu.VMEM((8, 40, 128), F32), dma((5,)),
                        dma((2, n, 3)), dma((8,)), dma((2, n, 4)), dma((2, n, 5)),
                        dma((2, n, 3)), dma((8,)), dma((2, n, 4)), dma((2, n, 5)), dma((2, n))],
        compiler_params=pltpu.CompilerParams(collective_id=0, has_side_effects=True, vmem_limit_bytes=20 << 20),
        name="gather_nodes",
    )(*(pltpu.with_memory_space_constraint(a, pltpu.HBM) for a in (nodes, pos, slots, counts, lists)))


WIDE = 3
def halves(v):
    a = v.astype(BF16)
    return a, (v - a.astype(F32)).astype(BF16)

def force_kernel(counts_vmem, lists_vmem, nodes, feats, where_p, slot16, out_ref, sb, cols, high, low, total, forces, counts, lists, sems):
    fetch = [pltpu.make_async_copy(counts_vmem, counts, sems.at[0]), pltpu.make_async_copy(lists_vmem, lists, sems.at[1])]
    for cp in fetch:
        cp.start()
    own_z = (lax.axis_index("gy") >> 1) & 7
    for cp in fetch:
        cp.wait()
    total[...] = jnp.zeros_like(total)
    def block_row(b):
        d = b >> 2
        c, z = d & 1, ((d >> 1) - own_z) & 7
        z = jnp.where(z > 4, 16 - 2 * z, jnp.maximum(2 * z - 1, 0))
        x, y = ((d >> 3) & 2) | ((d >> 7) & 1), (d >> 5) & 3
        p = jnp.where(c == 0, x, y)
        q = jnp.where(c == 0, y, x)
        return ((((c * 4 + q) * 8 + z) * 4 + p) * 4 + (b & 3)) * 16

    live = lax.fori_loop(0, TILES, lambda t, n: n + counts[t], 0)

    def take(t, k):
        ok = t < TILES
        at = jnp.minimum(t, TILES - 1)
        row = block_row(jnp.where(ok, lists[at, k], 0))
        last = k + 1 >= counts[at]
        return (row, t), (jnp.where(ok & last, t + 1, t), jnp.where(last, 0, k + 1))

    def node_at(row):
        return nodes[pl.ds(pl.multiple_of(row, 16), 16), :]

    def sums(h, pair):
        hi, lo = halves(node_at(pair[0]))
        both = jnp.concatenate([hi, lo], axis=0)
        return (jnp.dot(both, high[h], preferred_element_type=F32)
                + jnp.dot(both.astype(F32), low[h], preferred_element_type=F32))

    def radial(h):
        for r in range(0, 128, 8):
            dist = sb[h, r:r + 8, 0:128]
            mass = jnp.broadcast_to(cols[h, r:r + 8, 15:16], (8, 128))
            trace = jnp.broadcast_to(cols[h, r:r + 8, 11:12], (8, 128))
            w = lax.rsqrt(dist)
            u = w * w
            v = jnp.exp2(-dist) * u
            top = w + TOP[3]
            for coef in TOP[2::-1]:
                top = top * w + coef
            bottom = w + BOTTOM[2]
            for coef in BOTTOM[1::-1]:
                bottom = bottom * w + coef
            f0 = top * pl.reciprocal(bottom)
            f1 = f0 * u + FIRST
            f2 = f1 * u + SECOND
            both = (v * (mass * f0 + trace * f1 + sb[h, r:r + 8, 128:256] * f2), v * f1)
            for k, val in enumerate(both):
                hi = val.astype(BF16)
                high[h, r:r + 8, k * 128:k * 128 + 128] = hi
                low[h, r:r + 8, k * 128:k * 128 + 128] = val - hi.astype(F32)

    def products(h, pair):
        row, t = pair
        node = node_at(row)
        p1, p2, p3 = thirds(node)
        sb[h] = jnp.dot(jnp.concatenate([p1, p2, p3, p1, p2, p1], axis=0).T, feats[jnp.minimum(t, TILES - 1)], preferred_element_type=F32)
        cols[h, :, 0:16] = node.T

    idle = ((0, TILES),) * WIDE

    def pair_step(i, carry):
        at, first, second, third = carry
        got = [sums(h, third[h]) for h in range(WIDE)]
        for h in range(WIDE):
            radial(h)
        for h in range(WIDE):
            products(h, first[h])
        for h in range(WIDE):
            total[third[h][1]] += got[h]
        fresh = []
        for h in range(WIDE):
            pair, at = take(*at)
            fresh.append(pair)
        return at, tuple(fresh), first, second
    at = (0, 0)
    begin = []
    for h in range(WIDE):
        pair, at = take(*at)
        begin.append(pair)
    lax.fori_loop(0, (live + WIDE - 1) // WIDE + 2, pair_step, (at, tuple(begin), idle, idle))

    for t in range(TILES):
        s = total[t, 0:16, :] + total[t, 16:32, :]
        x, y, z = where_p[t, 0:1, :], where_p[t, 1:2, :], where_p[t, 2:3, :]
        rad = lambda k: s[k:k + 1, 0:128]
        sec = lambda k: s[k:k + 1, 128:256] * (SCALE * RATE**2)
        m = rad(4)
        xx, yy, xy, xz, yz = sec(9), sec(10), sec(12), sec(13), sec(14)
        zz = 2.0 * s[11:12, 128:256] - xx - yy
        forces[0, t:t + 1, :] = x * m - rad(0) + xx * x + xy * y + xz * z - sec(5)
        forces[1, t:t + 1, :] = y * m - rad(1) + xy * x + yy * y + yz * z - sec(6)
        forces[2, t:t + 1, :] = z * m - rad(2) + xz * x + yz * y + zz * z - sec(7)
    slot = slot16[...]
    at = slot % 128
    tile = slot // 128
    for k in range(3):
        got = jnp.zeros((16, 128), F32)
        for t in range(TILES):
            row = jnp.broadcast_to(forces[k, t:t + 1, :], (16, 128))
            got = jnp.where(tile == t, jnp.take_along_axis(row, at, axis=1), got)
        for r in range(16):
            out_ref[k:k + 1, r * 128:(r + 1) * 128] = got[r:r + 1, :]

def forces_of(counts, lists, nodes, feats, where_p, slots):
    vmem = pl.BlockSpec(memory_space=pltpu.VMEM)
    return pl.pallas_call(
        force_kernel,
        out_shape=jax.ShapeDtypeStruct((3, TILES * TILE), F32),
        in_specs=[vmem] * 6,
        out_specs=vmem,
        scratch_shapes=[pltpu.VMEM((WIDE, 128, 256), F32), pltpu.VMEM((WIDE, 128, 128), F32),
                        pltpu.VMEM((WIDE, 128, 256), BF16), pltpu.VMEM((WIDE, 128, 256), F32), pltpu.VMEM((17, 32, 256), F32), pltpu.VMEM((3, 16, 128), F32),
                        pltpu.SMEM((16,), jnp.int32), pltpu.SMEM((16, 16), jnp.int32), pltpu.SemaphoreType.DMA((2,))],
        compiler_params=pltpu.CompilerParams(vmem_limit_bytes=16 << 20),
        name="tile_forces",
    )(counts, lists, nodes, feats, where_p, slots)


def shards(positions, node_moments, slot_of, block_list, tile_counts):
    nodes, feats, where_p, slots, counts, lists = gather_nodes(
        node_moments, positions, slot_of, tile_counts, block_list
    )
    return forces_of(counts, lists, nodes, feats, where_p, slots)


def solution(mesh):
    placed = (
        P(None, ("gx", "gy")),
        P(None, ("gx", "gy")),
        P(("gx", "gy"), None),
        P(("gx", "gy"), None),
        P(("gx", "gy")),
    )
    return jax.shard_map(
        shards, mesh=mesh, in_specs=placed, out_specs=P(None, ("gx", "gy")), check_vma=False
    )
```

```python
import functools
import math

import jax
import jax.numpy as jnp
from jax import lax
from jax.experimental import pallas as pl
from jax.experimental.pallas import tpu as pltpu
from jax.sharding import PartitionSpec as P

F32 = jnp.float32
BF16 = jnp.bfloat16
TILE = 128
TILES = 16
RATE = 0.25 * math.log2(math.e)
SCALE = 3.00002466 * math.sqrt(RATE)
TOP = (0.137173002, 0.67870502, 1.41669777, 1.3963634)
BOTTOM = (0.145984292, 0.723140227, 1.39646547)
ROOT_PI = math.sqrt(math.pi)
FIRST = 0.5 / ROOT_PI / (SCALE * RATE)
SECOND = 0.05 / ROOT_PI / (SCALE * RATE**2)
MESH = pl.DeviceIdType.MESH
NZ = 8
NR = 4

def thirds(v):
    a = v.astype(BF16)
    r = v - a.astype(F32)
    b = r.astype(BF16)
    return a, b, (r - b.astype(F32)).astype(BF16)

def particle_rows(pos):
    x = pos[0:1] - 2.0
    y = pos[1:2] - 2.0
    z = pos[2:3] - 2.0
    none = jnp.zeros_like(x)
    xx, yy, zz = x * x, y * y, z * z
    g = -2.5 * SCALE * RATE**3
    dist = [-2.0 * RATE * x, -2.0 * RATE * y, -2.0 * RATE * z, none + RATE, RATE * (xx + yy + zz)] + [none] * 11
    quad = [none] * 5 + [-2.0 * g * x, -2.0 * g * y, -2.0 * g * z, none + g, g * (xx - zz), g * (yy - zz), -5.0 * RATE * zz,
            2.0 * g * (x * y), 2.0 * g * (x * z), 2.0 * g * (y * z), none]
    return jnp.concatenate(dist + quad, axis=0)

def node_rows(v):
    mass = v[0]
    x, y, z = v[1] - 2.0, v[2] - 2.0, v[3] - 2.0
    qxx, qyy, qzz, qxy, qxz, qyz = v[4:]
    qcx = qxx * x + qxy * y + qxz * z
    qcy = qxy * x + qyy * y + qyz * z
    qcz = qxz * x + qyz * y + qzz * z
    return [x, y, z, x * x + y * y + z * z + 0.25, jnp.ones_like(x), qcx, qcy, qcz,
            x * qcx + y * qcy + z * qcz, qxx, qyy, (0.5 * SCALE * RATE**2) * (qxx + qyy + qzz), qxy, qxz, qyz,
            (-SCALE * RATE / 3.0) * mass]

def device_of(first, p, q, z, c):
    x = first * p + (1 - first) * q
    y = first * q + (1 - first) * p
    return (lax.rem(x, 2) * 4 + y, (x // 2) * 16 + z * 2 + c)

ZPOS = (0, 1, 3, 5, 7, 6, 4, 2)
GROUPS = ((0, 1), (1, 3), (3, 6), (6, 8))
P_STEPS = ((0, 1), (1, 3), (2, 2))
Z_STEPS = (1, 7, 2, 6, 3, 5, 4)

def gather_kernel(nodes_hbm, pos_hbm, slot_hbm, counts_hbm, lists_hbm, nodes, feats, where_p, slot16, counts, lists,
                  v3, v2, own_ref, pos_ref, slot_ref, rows_p, slot_col, stage, load_sem, pin_sem, zin_sem, qin_sem, cin_sem, psend, zsend, qsend, csend, own_sem):
    gx = lax.axis_index("gx")
    gy = lax.axis_index("gy")
    c = lax.rem(gy, 2)
    z = lax.rem(gy // 2, 8)
    x = (gy // 16) * 2 + gx // 4
    y = lax.rem(gx, 4)
    refs = (v3, v2)
    rows = ((0, 24), (24, 16))
    firsts = (1 - c, c)
    ps = tuple(f * x + (1 - f) * y for f in firsts)
    qs = tuple(f * y + (1 - f) * x for f in firsts)

    def dev(s, p, q, zz, cc):
        return device_of(firsts[s], lax.rem(p, 4), lax.rem(q, 4), lax.rem(zz, 8), cc)

    def qat(s, rel):
        return lax.rem(qs[s] + rel, 4)

    def span(g):
        lo, hi = GROUPS[g]
        return pl.ds(lo, hi - lo)

    for q in range(10):
        for b in range(4):
            pltpu.make_async_copy(nodes_hbm.at[pl.ds(q, 1), pl.ds(b * 128, 128)], own_ref.at[pl.ds(q * 4 + b, 1)], load_sem.at[0]).start()
    fetch = [pltpu.make_async_copy(pos_hbm, pos_ref, load_sem.at[1]), pltpu.make_async_copy(slot_hbm, slot_ref, load_sem.at[2]),
             pltpu.make_async_copy(counts_hbm, counts, load_sem.at[3]), pltpu.make_async_copy(lists_hbm, lists, load_sem.at[4])]
    for cp in fetch:
        cp.start()

    barrier = pltpu.get_barrier_semaphore()
    peers = [device_of(1, x, y, z, 1 - c)]
    for d in (1, 2, 3):
        peers.append(device_of(1, lax.rem(x + d, 4), y, z, c))
        peers.append(device_of(1, x, lax.rem(y + d, 4), z, c))
    for d in range(1, 8):
        peers.append(device_of(1, x, y, lax.rem(z + d, 8), c))
    for peer in peers:
        pl.semaphore_signal(barrier, inc=1, device_id=peer, device_id_type=MESH)
    pltpu.make_async_copy(own_ref, own_ref, load_sem.at[0]).wait()
    pl.semaphore_wait(barrier, len(peers))

    sends = []

    def send(src, dst, ssem, rsem, to):
        cp = pltpu.make_async_remote_copy(src_ref=src, dst_ref=dst, send_sem=ssem, recv_sem=rsem, device_id=to, device_id_type=MESH)
        cp.start()
        sends.append(cp)

    def arrived(ref, sem):
        pltpu.make_async_remote_copy(src_ref=ref, dst_ref=ref, send_sem=sem, recv_sem=sem, device_id=(gx, gy), device_id_type=MESH).wait_recv()

    for d in Z_STEPS:
        pos = ZPOS[8 - d]
        send(own_ref, stage.at[pos], zsend.at[pos], zin_sem.at[pos], dev(0, ps[0], qs[0], z + d, c))
    local = {}

    def column(g):
        lo, hi = GROUPS[g]
        for pos in range(max(lo, 1), hi):
            arrived(stage.at[pos], zin_sem.at[pos])
        for s in (0, 1):
            r0, rn = rows[s]
            src = own_ref.at[pl.ds(r0, rn)] if hi == 1 else stage.at[span(g), pl.ds(r0, rn)]
            at = 0 if hi == 1 else span(g)
            dst = refs[s].at[c, qs[s], at, ps[s]]
            for i, d in P_STEPS:
                send(src, dst, psend.at[s, g, i], pin_sem.at[s, g, i], dev(s, ps[s] + d, qs[s], z, c))
            cp = pltpu.make_async_copy(src, dst, own_sem.at[s, g])
            cp.start()
            local[s, g] = cp

    def bundle(s, qrel, g):
        return refs[s].at[c, qat(s, qrel), span(g)]

    def ready(g):
        lo, hi = GROUPS[g]
        for s in (0, 1):
            for i, d in P_STEPS:
                at = 0 if hi == 1 else span(g)
                arrived(refs[s].at[c, qs[s], at, lax.rem(ps[s] + 4 - d, 4)], pin_sem.at[s, g, i])
            local[s, g].wait()
            b = bundle(s, 0, g)
            send(b, b, qsend.at[s, g, 0], qin_sem.at[s, g, 0], dev(s, ps[s], qs[s] + 1, z, c))
            send(b, b, qsend.at[s, g, 1], qin_sem.at[s, g, 1], dev(s, ps[s], qs[s] + 3, z, c))
            send(b, b, csend.at[s, g, 0], cin_sem.at[s, g, 0], dev(s, ps[s], qs[s], z, 1 - c))

    def side(g):
        for s in (0, 1):
            for i, rel in ((0, 3), (1, 1)):
                b = bundle(s, rel, g)
                arrived(b, qin_sem.at[s, g, i])
                h = refs[s].at[c, qat(s, rel), span(g), pl.ds(2 * i, 2)]
                send(h, h, qsend.at[s, g, 2 + i], qin_sem.at[s, g, 2 + i], dev(s, ps[s], qs[s] + (1 if i == 0 else 3), z, c))
        for s in (0, 1):
            for i, rel in ((0, 3), (1, 1)):
                b = bundle(s, rel, g)
                send(b, b, csend.at[s, g, 1 + i], cin_sem.at[s, g, 1 + i], dev(s, ps[s], qs[s], z, 1 - c))

    def far(g):
        for s in (0, 1):
            for i in (0, 1):
                h = refs[s].at[c, qat(s, 2), span(g), pl.ds(2 * i, 2)]
                arrived(h, qin_sem.at[s, g, 2 + i])
                send(h, h, csend.at[s, g, 3 + i], cin_sem.at[s, g, 3 + i], dev(s, ps[s], qs[s], z, 1 - c))

    tiles_done = [0]

    def particle_prep():
        for cp in fetch:
            cp.wait()
        for r in range(16):
            slot16[r:r + 1, :] = slot_ref[0:1, r * 128:(r + 1) * 128]
        slot_t = slot16[...].T
        for r in range(16):
            slot_col[r] = jnp.broadcast_to(slot_t[:, r:r + 1], (128, 128))
        for i, piece in enumerate(thirds(particle_rows(pos_ref[...]))):
            rows_p[i * 32:(i + 1) * 32, :] = piece

    lane = lax.broadcasted_iota(jnp.int32, (128, 128), 1)

    def tile_step(t, _):
        base = lane + t * 128
        acc = jnp.zeros((96, 128), F32)
        for r in range(0, 16, 2):
            hot = jnp.concatenate([(slot_col[r + h] == base).astype(F32).astype(BF16) for h in (0, 1)], axis=0)
            acc = acc + jnp.dot(rows_p[:, r * 128:(r + 2) * 128], hot, preferred_element_type=F32)
        got = acc.astype(BF16)
        for g, piece in enumerate((0, 0, 0, 1, 1, 2)):
            feats[t, g * 16:(g + 1) * 16, 0:128] = got[piece * 32:piece * 32 + 16]
            feats[t, g * 16:(g + 1) * 16, 128:256] = got[piece * 32 + 16:piece * 32 + 32]
        where_p[t] = (-0.5 / RATE) * (acc[0:8] + acc[32:40] + acc[64:72])
        return 0

    def particle_tiles(n):
        lax.fori_loop(tiles_done[0], tiles_done[0] + n, tile_step, 0)
        tiles_done[0] += n

    def partner(g):
        for s in (0, 1):
            for k, qrel in enumerate((0, 3, 1)):
                qp = lax.rem(qs[1 - s] + qrel, 4)
                arrived(refs[s].at[1 - c, qp, span(g)], cin_sem.at[s, g, k])
            for i in (0, 1):
                qp = lax.rem(qs[1 - s] + 2, 4)
                arrived(refs[s].at[1 - c, qp, span(g), pl.ds(2 * i, 2)], cin_sem.at[s, g, 3 + i])

    def features(core, g):
        lo, hi = GROUPS[g]

        def step(j, _):
            at = lo + j
            for q in range(4):
                for p in (0, 2):
                    vals = []
                    for k in range(10):
                        if k < 6:
                            a, b = v3[core, q, at, p, 4 * k:4 * k + 4, :], v3[core, q, at, p + 1, 4 * k:4 * k + 4, :]
                        else:
                            r = 4 * k - 24
                            a, b = v2[core, p, at, q, r:r + 4, :], v2[core, p + 1, at, q, r:r + 4, :]
                        vals.append(jnp.concatenate([a, b], axis=0))
                    base = pl.multiple_of(((core * 4 + q) * 8 + at) * 256 + p * 64, 128)
                    for f, row in enumerate(node_rows(vals)):
                        nodes[pl.ds(base + f, 8, stride=16), :] = row
            return 0
        lax.fori_loop(0, hi - lo, step, 0)

    column(0)
    particle_prep()
    particle_tiles(8)
    column(1)
    particle_tiles(2)
    column(2)
    column(3)
    ready(0)
    ready(1)
    particle_tiles(2)
    ready(2)
    particle_tiles(2)
    ready(3)
    particle_tiles(2)
    side(0)
    side(1)
    side(2)
    side(3)
    far(0)
    features(c, 0)
    far(1)
    features(c, 1)
    far(2)
    far(3)
    features(c, 2)
    partner(0)
    features(1 - c, 0)
    partner(1)
    features(1 - c, 1)
    partner(2)
    features(1 - c, 2)
    features(c, 3)
    partner(3)
    features(1 - c, 3)
    for cp in sends:
        cp.wait_send()

def gather_nodes(nodes, pos, slots, counts, lists):
    dma = pltpu.SemaphoreType.DMA
    n = len(GROUPS)
    vmem = pl.BlockSpec(memory_space=pltpu.VMEM)
    hbm = pl.BlockSpec(memory_space=pltpu.HBM)
    return pl.pallas_call(
        gather_kernel,
        out_shape=[jax.ShapeDtypeStruct((1024 * 16, 128), F32),
                   jax.ShapeDtypeStruct((TILES, 96, 256), BF16),
                   jax.ShapeDtypeStruct((TILES, 8, 128), F32),
                   jax.ShapeDtypeStruct((16, 128), jnp.int32),
                   jax.ShapeDtypeStruct(counts.shape, jnp.int32),
                   jax.ShapeDtypeStruct(lists.shape, jnp.int32)],
        in_specs=[hbm] * 5,
        out_specs=[vmem] * 6,
        scratch_shapes=[pltpu.VMEM((2, NR, NZ, NR, 24, 128), F32), pltpu.VMEM((2, NR, NZ, NR, 16, 128), F32),
                        pltpu.VMEM((40, 128), F32), pltpu.VMEM((3, 2048), F32), pltpu.VMEM((1, 2048), jnp.int32),
                        pltpu.VMEM((96, 2048), BF16), pltpu.VMEM((16, 128, 128), jnp.int32),
                        pltpu.VMEM((8, 40, 128), F32), dma((5,)),
                        dma((2, n, 3)), dma((8,)), dma((2, n, 4)), dma((2, n, 5)),
                        dma((2, n, 3)), dma((8,)), dma((2, n, 4)), dma((2, n, 5)), dma((2, n))],
        compiler_params=pltpu.CompilerParams(collective_id=0, has_side_effects=True, vmem_limit_bytes=20 << 20),
        name="gather_nodes",
    )(*(pltpu.with_memory_space_constraint(a, pltpu.HBM) for a in (nodes, pos, slots, counts, lists)))


WIDE = 3
def halves(v):
    a = v.astype(BF16)
    return a, (v - a.astype(F32)).astype(BF16)

def force_kernel(counts_vmem, lists_vmem, nodes, feats, where_p, slot16, out_ref, sb, cols, high, low, total, forces, counts, lists, sems):
    fetch = [pltpu.make_async_copy(counts_vmem, counts, sems.at[0]), pltpu.make_async_copy(lists_vmem, lists, sems.at[1])]
    for cp in fetch:
        cp.start()
    own_z = (lax.axis_index("gy") >> 1) & 7
    for cp in fetch:
        cp.wait()
    total[...] = jnp.zeros_like(total)
    def block_row(b):
        d = b >> 2
        c, z = d & 1, ((d >> 1) - own_z) & 7
        z = jnp.where(z > 4, 16 - 2 * z, jnp.maximum(2 * z - 1, 0))
        x, y = ((d >> 3) & 2) | ((d >> 7) & 1), (d >> 5) & 3
        p = jnp.where(c == 0, x, y)
        q = jnp.where(c == 0, y, x)
        return ((((c * 4 + q) * 8 + z) * 4 + p) * 4 + (b & 3)) * 16

    live = lax.fori_loop(0, TILES, lambda t, n: n + counts[t], 0)

    def take(t, k):
        ok = t < TILES
        at = jnp.minimum(t, TILES - 1)
        row = block_row(jnp.where(ok, lists[at, k], 0))
        last = k + 1 >= counts[at]
        return (row, t), (jnp.where(ok & last, t + 1, t), jnp.where(last, 0, k + 1))

    def node_at(row):
        return nodes[pl.ds(pl.multiple_of(row, 16), 16), :]

    def sums(h, pair):
        hi, lo = halves(node_at(pair[0]))
        both = jnp.concatenate([hi, lo], axis=0)
        return (jnp.dot(both, high[h], preferred_element_type=F32)
                + jnp.dot(both.astype(F32), low[h], preferred_element_type=F32))

    def radial(h):
        for r in range(0, 128, 8):
            dist = sb[h, r:r + 8, 0:128]
            mass = jnp.broadcast_to(cols[h, r:r + 8, 15:16], (8, 128))
            trace = jnp.broadcast_to(cols[h, r:r + 8, 11:12], (8, 128))
            w = lax.rsqrt(dist)
            u = w * w
            v = jnp.exp2(-dist) * u
            top = w + TOP[3]
            for coef in TOP[2::-1]:
                top = top * w + coef
            bottom = w + BOTTOM[2]
            for coef in BOTTOM[1::-1]:
                bottom = bottom * w + coef
            f0 = top * pl.reciprocal(bottom)
            f1 = f0 * u + FIRST
            f2 = f1 * u + SECOND
            both = (v * (mass * f0 + trace * f1 + sb[h, r:r + 8, 128:256] * f2), v * f1)
            for k, val in enumerate(both):
                hi = val.astype(BF16)
                high[h, r:r + 8, k * 128:k * 128 + 128] = hi
                low[h, r:r + 8, k * 128:k * 128 + 128] = val - hi.astype(F32)

    def products(h, pair):
        row, t = pair
        node = node_at(row)
        p1, p2, p3 = thirds(node)
        sb[h] = jnp.dot(jnp.concatenate([p1, p2, p3, p1, p2, p1], axis=0).T, feats[jnp.minimum(t, TILES - 1)], preferred_element_type=F32)
        cols[h, :, 0:16] = node.T

    idle = ((0, TILES),) * WIDE

    def pair_step(i, carry):
        at, first, second, third = carry
        got = [sums(h, third[h]) for h in range(WIDE)]
        for h in range(WIDE):
            radial(h)
        for h in range(WIDE):
            products(h, first[h])
        for h in range(WIDE):
            total[third[h][1]] += got[h]
        fresh = []
        for h in range(WIDE):
            pair, at = take(*at)
            fresh.append(pair)
        return at, tuple(fresh), first, second
    at = (0, 0)
    begin = []
    for h in range(WIDE):
        pair, at = take(*at)
        begin.append(pair)
    lax.fori_loop(0, (live + WIDE - 1) // WIDE + 2, pair_step, (at, tuple(begin), idle, idle))

    for t in range(TILES):
        s = total[t, 0:16, :] + total[t, 16:32, :]
        x, y, z = where_p[t, 0:1, :], where_p[t, 1:2, :], where_p[t, 2:3, :]
        rad = lambda k: s[k:k + 1, 0:128]
        sec = lambda k: s[k:k + 1, 128:256] * (SCALE * RATE**2)
        m = rad(4)
        xx, yy, xy, xz, yz = sec(9), sec(10), sec(12), sec(13), sec(14)
        zz = 2.0 * s[11:12, 128:256] - xx - yy
        forces[0, t:t + 1, :] = x * m - rad(0) + xx * x + xy * y + xz * z - sec(5)
        forces[1, t:t + 1, :] = y * m - rad(1) + xy * x + yy * y + yz * z - sec(6)
        forces[2, t:t + 1, :] = z * m - rad(2) + xz * x + yz * y + zz * z - sec(7)
    slot = slot16[...]
    at = slot % 128
    tile = slot // 128
    for k in range(3):
        got = jnp.zeros((16, 128), F32)
        for t in range(TILES):
            row = jnp.broadcast_to(forces[k, t:t + 1, :], (16, 128))
            got = jnp.where(tile == t, jnp.take_along_axis(row, at, axis=1), got)
        for r in range(16):
            out_ref[k:k + 1, r * 128:(r + 1) * 128] = got[r:r + 1, :]

def forces_of(counts, lists, nodes, feats, where_p, slots):
    vmem = pl.BlockSpec(memory_space=pltpu.VMEM)
    return pl.pallas_call(
        force_kernel,
        out_shape=jax.ShapeDtypeStruct((3, TILES * TILE), F32),
        in_specs=[vmem] * 6,
        out_specs=vmem,
        scratch_shapes=[pltpu.VMEM((WIDE, 128, 256), F32), pltpu.VMEM((WIDE, 128, 128), F32),
                        pltpu.VMEM((WIDE, 128, 256), BF16), pltpu.VMEM((WIDE, 128, 256), F32), pltpu.VMEM((17, 32, 256), F32), pltpu.VMEM((3, 16, 128), F32),
                        pltpu.SMEM((16,), jnp.int32), pltpu.SMEM((16, 16), jnp.int32), pltpu.SemaphoreType.DMA((2,))],
        compiler_params=pltpu.CompilerParams(vmem_limit_bytes=16 << 20),
        name="tile_forces",
    )(counts, lists, nodes, feats, where_p, slots)


def shards(positions, node_moments, slot_of, block_list, tile_counts):
    nodes, feats, where_p, slots, counts, lists = gather_nodes(
        node_moments, positions, slot_of, tile_counts, block_list
    )
    return forces_of(counts, lists, nodes, feats, where_p, slots)


def solution(mesh):
    placed = (
        P(None, ("gx", "gy")),
        P(None, ("gx", "gy")),
        P(("gx", "gy"), None),
        P(("gx", "gy"), None),
        P(("gx", "gy")),
    )
    return jax.shard_map(
        shards, mesh=mesh, in_specs=placed, out_specs=P(None, ("gx", "gy")), check_vma=False
    )
```
